128 devices in a mesh: tx: 8 (over z, core), ty: 16 (over x, y).
Axes of the slice: x: 4, y: 4, z: 4, core: 2. Of those that a mesh axis runs over, the one named last changes fastest.
Arguments:
- frames: bfloat16 [8, 48, 1, 5, 384, 384], P('tx', 'ty'), may hold values from -6 to 6
- masks: int32 [8, 48, 12, 12], P('tx', 'ty'), may hold values 0 or 1
- phases: float32 [8, 48, 1], P('tx', 'ty'), may hold values from -3.140625 to 3.140625
- slot_tile: int32 [8, 48], P('tx', 'ty'), may hold values from -1 to 31, as said below
- otf: float32 [384, 384], replicated, may hold values from 0.05 to 1
- apod: float32 [384, 384], replicated, may hold values from 0.2 to 1
Outputs:
- stitched: float32 [5120, 5120], P('ty', 'tx')
The draws below stay inside these ranges and needn't reach their ends.
Inputs may be any that keep to these rules, and one draw needn't show every extreme that they name: `slot_tile`: in each column of devices, every tile is held in exactly one slot and is named 2 h + c for its tile row h and its tile column c within that column of devices; -1 marks an empty slot. The slots of one device never hold two tiles of the same tile row. In every draw some devices of every column hold 3 tiles.
All inputs are finite; a program needn't handle non-finite values. No bound on the sum of `masks` on one device may be relied on, other than what follows from the above.
Results may differ from the reference program's by a relative error of at most 0.0068.
Values may be sent and summed in bfloat16 or wider, within the bound.
No kernel may reach another device: no remote copies, remote signals or barrier semaphores. Data moves between devices by JAX's collectives and lax.ppermute only.
A program may use at most 128 MiB of HBM per device.

```python
import math
import jax
import jax.numpy as jnp
from jax import lax

TILE_SIDE = 384
STRIDE = 320
ORIENT = 1
PHASES = 5
GROUP_COLS = 2
TILE_ROWS = 16
GROUPS = 8
SLOTS = 48
MASK_CELLS = 12
N_TY = 16


def shuffle_row(row_key):
    return jax.random.permutation(row_key, 3)


def group_table(group_key):
    first, second, third = jax.random.split(group_key, 3)
    worker_order = jax.random.permutation(first, TILE_ROWS)
    offset = 2 * jax.random.randint(second, (), 1, TILE_ROWS // 2)
    places = jnp.arange(TILE_ROWS, dtype=jnp.int32)
    start_row = (places - offset) % TILE_ROWS
    is_even = places % 2 == 0
    own_tile = 2 * places
    extra_one = jnp.where(is_even, 2 * start_row + 1, -1)
    extra_two = jnp.where(is_even, 2 * start_row + 3, -1)
    rows_by_place = jnp.stack([own_tile, extra_one, extra_two], axis=1)
    inverse = jnp.argsort(worker_order)
    slot_table = rows_by_place[inverse]
    row_keys = jax.random.split(third, TILE_ROWS)
    shuffle = jax.vmap(shuffle_row)(row_keys)
    slot_table = jnp.take_along_axis(slot_table, shuffle, axis=1)
    return slot_table.reshape(-1).astype(jnp.int32)


def draw_slot_tile(key, part):
    group_keys = jax.random.split(jax.random.fold_in(key, 17), GROUPS)
    return jax.vmap(group_table)(group_keys)


def with_ends(entries, key, low, top_value):
    shape = entries.shape
    index_at = [jax.random.randint(jax.random.fold_in(key, axis), (), 0, shape[axis]) for axis in range(len(shape))]
    entries = entries.at[tuple(index_at)].set(low)
    longest = shape.index(max(shape))
    index_at[longest] = (index_at[longest] + 1) % shape[longest]
    return entries.at[tuple(index_at)].set(top_value)


def block_levels(rng, dims, cuts, least, largest):
    def one(position, parts):
        draws = jax.random.uniform(jax.random.fold_in(jax.random.fold_in(rng, 6), position), (parts,), jnp.float32, least / len(cuts), largest / len(cuts))
        return jnp.repeat(jnp.exp(draws), dims[position] // parts).reshape((-1,) + (1,) * (len(dims) - position - 1))

    factor_of = one(*cuts[0])
    for cut in cuts[1:]:
        factor_of = factor_of * one(*cut)
    return factor_of


def normal_values(key, dims, spread, reach, shards=(), kind=jnp.bfloat16):
    drawn = spread * jax.random.normal(key, dims, jnp.float32)
    if shards:
        drawn = drawn * block_levels(key, dims, shards, -0.22, 0.18)
    return jnp.clip(drawn, -reach, reach).astype(kind)


def setup_inputs(seed: int = 0) -> dict:
    key_of = jax.random.split(jax.random.key(seed), 7)
    frames = normal_values(key_of[0], (GROUPS, SLOTS, ORIENT, PHASES, TILE_SIDE, TILE_SIDE), 1.0, 6.0, ((0, 8), (1, 16)))
    masks = with_ends((jax.random.randint(key_of[1], (GROUPS, SLOTS, MASK_CELLS, MASK_CELLS), 0, 4) < 3).astype(jnp.int32), jax.random.fold_in(key_of[1], 1), 0, 1)
    phases = jnp.clip(jax.random.uniform(key_of[2], (GROUPS, SLOTS, ORIENT), jnp.float32, -3.140625, 3.140625), -3.140625, 3.140625)
    slot_tile = draw_slot_tile(jax.random.fold_in(key_of[6], 71), 0)
    otf = jnp.clip(jnp.exp(jax.random.uniform(key_of[4], (TILE_SIDE, TILE_SIDE), jnp.float32, math.log(0.05), math.log(1.0))), 0.05, 1.0)
    apod = jnp.clip(jnp.exp(jax.random.uniform(key_of[5], (TILE_SIDE, TILE_SIDE), jnp.float32, math.log(0.2), math.log(1.0))), 0.2, 1.0)
    return dict(frames=frames, masks=masks, phases=phases, slot_tile=slot_tile, otf=otf, apod=apod)


wiener = 0.1
pattern_base = (37, 101)
pattern_step = (29, -53)


def batched(pattern, operand_a, operand_b):
    return jnp.einsum(pattern, operand_a.astype(jnp.float32), operand_b.astype(jnp.float32), precision=lax.Precision.HIGHEST)


def plain_dot(operand_a, operand_b):
    return jnp.dot(operand_a.astype(jnp.float32), operand_b.astype(jnp.float32), precision=lax.Precision.HIGHEST)


def mix_bands(pattern, operand_a, operand_b):
    return jnp.einsum(pattern, operand_a, operand_b, precision=lax.Precision.HIGHEST)


def dft_tables(length):
    places = jnp.arange(length, dtype=jnp.int32)
    product = (places[:, None] * places[None, :]) % length
    angles = product.astype(jnp.float32) * (2.0 * math.pi / length)
    return jnp.cos(angles).astype(jnp.bfloat16), jnp.sin(angles).astype(jnp.bfloat16)


def pattern_shift(orient):
    return (pattern_base[0] + orient * pattern_step[0], pattern_base[1] + orient * pattern_step[1])


def filter_weights(otf, apod, orient_count, phase_count):
    halfway = phase_count // 2
    rolled = []
    for orient in range(orient_count):
        shift_rows, shift_cols = pattern_shift(orient)
        for band_place in range(phase_count):
            band_order = band_place - halfway
            rolled.append(jnp.roll(otf, (-band_order * shift_rows, -band_order * shift_cols), (0, 1)))
    rolled_stack = jnp.stack(rolled)
    denominator = wiener + jnp.sum(rolled_stack * rolled_stack, axis=0)
    return rolled_stack * (apod / denominator)[None]


def tile_image(planes, cell_mask, offsets, gain_maps, cosine, sine_table):
    orient_count, phase_count, length = planes.shape[0], planes.shape[1], planes.shape[2]
    cell_count = cell_mask.shape[0]
    cell_width = length // cell_count
    shaped = planes.reshape(orient_count * phase_count, cell_count, cell_width, cell_count, cell_width)
    masked = (shaped * cell_mask.astype(jnp.bfloat16)[None, :, None, :, None]).reshape(orient_count * phase_count, length, length)
    first_real = batched("pjk,kl->pjl", masked, cosine).astype(jnp.bfloat16)
    first_imag = (-batched("pjk,kl->pjl", masked, sine_table)).astype(jnp.bfloat16)
    four_real = batched("jk,pkl->pjl", cosine, first_real) + batched("jk,pkl->pjl", sine_table, first_imag)
    four_imag = batched("jk,pkl->pjl", cosine, first_imag) - batched("jk,pkl->pjl", sine_table, first_real)
    halfway = phase_count // 2
    orders = jnp.arange(-halfway, halfway + 1).astype(jnp.float32)
    phase_steps = jnp.arange(phase_count).astype(jnp.float32) * (2.0 * math.pi / phase_count)
    spec_real = jnp.zeros((length, length), jnp.float32)
    spec_imag = jnp.zeros((length, length), jnp.float32)
    for orient in range(orient_count):
        shift_rows, shift_cols = pattern_shift(orient)
        angles = orders[:, None] * (offsets[orient] + phase_steps)[None, :]
        coef_real = jnp.cos(angles) / phase_count
        coef_imag = jnp.sin(angles) / phase_count
        part_real = four_real[orient * phase_count:(orient + 1) * phase_count]
        part_imag = four_imag[orient * phase_count:(orient + 1) * phase_count]
        band_real = mix_bands("mp,pxy->mxy", coef_real, part_real) + mix_bands("mp,pxy->mxy", coef_imag, part_imag)
        band_imag = mix_bands("mp,pxy->mxy", coef_real, part_imag) - mix_bands("mp,pxy->mxy", coef_imag, part_real)
        for band_place in range(phase_count):
            band_order = band_place - halfway
            offset_pair = (-band_order * shift_rows, -band_order * shift_cols)
            gain_map = gain_maps[orient * phase_count + band_place]
            spec_real = spec_real + gain_map * jnp.roll(band_real[band_place], offset_pair, (0, 1))
            spec_imag = spec_imag + gain_map * jnp.roll(band_imag[band_place], offset_pair, (0, 1))
    wave_real = spec_real.astype(jnp.bfloat16)
    wave_imag = spec_imag.astype(jnp.bfloat16)
    mid_real = (plain_dot(wave_real, cosine) - plain_dot(wave_imag, sine_table)).astype(jnp.bfloat16)
    mid_imag = (plain_dot(wave_real, sine_table) + plain_dot(wave_imag, cosine)).astype(jnp.bfloat16)
    return (plain_dot(cosine, mid_real) - plain_dot(sine_table, mid_imag)) * (1.0 / (length * length))


def ramp_weights(length, intersection, is_last):
    places = jnp.arange(length).astype(jnp.float32) + 0.5
    rising = jnp.minimum(places / intersection, 1.0)
    falling = jnp.minimum((length - places) / intersection, 1.0)
    return rising * jnp.where(is_last, jnp.ones_like(falling), falling)


def blended(picture, row_last, column_last, intersection):
    length = picture.shape[0]
    weighted = (picture * ramp_weights(length, intersection, row_last)[:, None]) * ramp_weights(length, intersection, column_last)[None, :]
    return weighted.astype(jnp.bfloat16)


def reference(frames, masks, phases, slot_tile, otf, apod):
    length = otf.shape[0]
    intersection = length - STRIDE
    group_count = frames.shape[0]
    row_count = N_TY
    tile_count = GROUP_COLS * row_count
    cosine, sine_table = dft_tables(length)
    gain_maps = filter_weights(otf, apod, frames.shape[2], frames.shape[3])
    slot_places = jnp.arange(frames.shape[1], dtype=jnp.int32)

    def locate(tile_list):
        target = jnp.where(tile_list >= 0, tile_list, tile_count).astype(jnp.int32)
        return jnp.zeros((tile_count,), jnp.int32).at[target].set(slot_places, mode="drop")

    slot_of = jax.vmap(locate)(slot_tile)
    canvas_full = jnp.zeros((STRIDE * row_count + intersection, STRIDE * GROUP_COLS * group_count + intersection), jnp.float32)

    def place_tile(number, canvas):
        group_id = (number // tile_count).astype(jnp.int32)
        tile_id = (number % tile_count).astype(jnp.int32)
        slot_id = slot_of[group_id, tile_id]
        picture = tile_image(frames[group_id, slot_id], masks[group_id, slot_id], phases[group_id, slot_id], gain_maps, cosine, sine_table)
        tile_row = tile_id // GROUP_COLS
        column = GROUP_COLS * group_id + tile_id % GROUP_COLS
        result = blended(picture, tile_row == row_count - 1, column == GROUP_COLS * group_count - 1, intersection)
        top_edge = (STRIDE * tile_row).astype(jnp.int32)
        left_edge = (STRIDE * column).astype(jnp.int32)
        region = lax.dynamic_slice(canvas, (top_edge, left_edge), (length, length))
        return lax.dynamic_update_slice(canvas, region + result.astype(jnp.float32), (top_edge, left_edge))

    canvas_full = lax.fori_loop(jnp.int32(0), jnp.int32(group_count * tile_count), place_tile, canvas_full)
    return canvas_full[intersection:, intersection:]
```

```python
import functools
import math

import jax
import jax.numpy as jnp
import numpy as np
from jax import lax
from jax.experimental import pallas as pl
from jax.experimental.pallas import tpu as pltpu
from jax.sharding import PartitionSpec as P

SIDE = 384
STRIDE = 320
OVERLAP = SIDE - STRIDE
GROUP_COLS = 2
PHASES = 5
WIENER = 0.1
SHIFT_ROWS, SHIFT_COLS = 37, 101
CHUNK = SIDE // 16
GROUP = 8

COL_A = np.arange(64, 128)
COL_B = np.arange(128, 192)
COL_C = np.arange(0, 64)
NYQUIST = SIDE // 2


def cos_sin(rows, cols):
    angle = (np.outer(rows, cols) % SIDE) * (2.0 * math.pi / SIDE)
    return np.cos(angle), np.sin(angle)


def first_table(order):
    n = np.arange(SIDE)

    def plus(cols):
        c, s = cos_sin(n, cols + order * SHIFT_COLS)
        return np.concatenate([c, -s]), np.concatenate([-s, -c])

    def minus(cols):
        c, s = cos_sin(n, cols - order * SHIFT_COLS)
        return np.concatenate([c, s]), np.concatenate([-s, c])

    blocks = [
        plus(COL_A), minus(COL_B), plus(COL_B), minus(COL_A),
        plus(COL_C), plus(np.array([NYQUIST])), minus(COL_C[1:]),
    ]
    return np.concatenate([b[0] for b in blocks] + [b[1] for b in blocks], axis=1)


def centre_table():
    n = np.arange(SIDE)
    cols = np.concatenate([COL_A, COL_B, COL_C, [NYQUIST]])
    c, s = cos_sin(n, cols)
    pad = np.zeros((SIDE, 63))
    return np.concatenate([c, pad, -s, pad], axis=1)


def forward_rows():
    c, s = cos_sin(np.arange(SIDE), np.arange(SIDE))
    return np.block([[c, s], [-s, c]])


def inverse_rows():
    c, s = cos_sin(np.arange(SIDE), np.arange(SIDE))
    return np.block([[c, -s], [s, c]])


def last_table():
    lines = np.concatenate([COL_A, COL_B, COL_C, [NYQUIST], COL_C[1:]])
    c, s = cos_sin(lines, np.arange(SIDE))
    return np.concatenate([c, -s], axis=0)


def table(values):
    return jnp.asarray(values.astype(np.float32)).astype(jnp.bfloat16)


def negated(array):
    return jnp.roll(array[::-1, ::-1], (1, 1), (0, 1))


def band_gains(otf, apod):
    halfway = PHASES // 2

    def weights(base, sign):
        moved = [
            jnp.roll(base, (-sign * m * SHIFT_ROWS, -sign * m * SHIFT_COLS), (0, 1))
            for m in range(-halfway, halfway + 1)
        ]
        total = WIENER + sum(one * one for one in moved)
        return moved, total

    moved, total = weights(otf, 1)
    back, back_total = weights(negated(otf), -1)
    scale = apod / total
    back_scale = negated(apod) / back_total

    gains = {}
    for m in range(-halfway, halfway + 1):
        gains[m] = moved[m + halfway] * scale + back[halfway - m] * back_scale

    tiles = []
    for m in (1, 2):
        up, down = gains[m], gains[-m]
        tiles += [
            up[:, 64:128], down[:, 128:192],
            up[:, 128:192], down[:, 64:128],
            up[:, 0:64], up[:, 192:193], down[:, 1:64],
        ]
    mid = gains[0]
    zeros = jnp.zeros((SIDE, 63), jnp.float32)
    tiles += [mid[:, 64:192], 0.5 * mid[:, 0:1], mid[:, 1:64], 0.5 * mid[:, 192:193], zeros]
    return jnp.concatenate(tiles, axis=1)


def tile_kernel(
    last_ref, frames_ref, masks_ref, turn_ref, gains_ref, rows_ref, cols_ref,
    w1_ref, w2_ref, w0_ref, fwd_ref, inv_ref, out_w_ref, out_ref, left_ref, y_ref, t_ref, s_ref,
):
    slot = pl.program_id(0)
    f32, bf16 = jnp.float32, jnp.bfloat16
    c1, c2 = math.cos(2 * math.pi / 5), math.cos(4 * math.pi / 5)
    n1, n2 = math.sin(2 * math.pi / 5), math.sin(4 * math.pi / 5)

    for cell in range(12):
        rows = pl.ds(32 * cell, 32)
        flag = masks_ref[0, cell : cell + 1, :]
        f = [frames_ref[0, p, rows, :].astype(f32) * flag for p in range(PHASES)]
        s1, d1, s2, d2 = f[1] + f[4], f[1] - f[4], f[2] + f[3], f[2] - f[3]
        left_ref[rows, 1536:1920] = ((f[0] + s1 + s2) * (1.0 / PHASES)).astype(bf16)
        for at, (a, b) in enumerate((
            (f[0] + c1 * s1 + c2 * s2, n1 * d1 + n2 * d2),
            (f[0] + c2 * s1 + c1 * s2, n2 * d1 - n1 * d2),
        )):
            c = turn_ref[0, rows, 2 * at : 2 * at + 1]
            s = turn_ref[0, rows, 2 * at + 1 : 2 * at + 2]
            left_ref[rows, 768 * at : 768 * at + 384] = (c * a - s * b).astype(bf16)
            left_ref[rows, 768 * at + 384 : 768 * at + 768] = (c * b + s * a).astype(bf16)

    def dot(x, w):
        return jnp.dot(x, w, preferred_element_type=f32)

    for at, w_ref in enumerate((w1_ref, w2_ref)):
        for part in range(3):
            lanes = pl.ds(256 * part, 256)
            r = dot(left_ref[:, 768 * at : 768 * at + 768], w_ref[:, lanes]).astype(bf16)
            for half in range(2):
                tile = 2 * part + half
                base = 384 if tile >= 3 else 0
                col = 384 * at + 128 * (tile % 3)
                y_ref[base : base + 384, col : col + 128] = r[:, 128 * half : 128 * half + 128]
    for part in range(2):
        r = dot(left_ref[:, 1536:1920], w0_ref[:, 256 * part : 256 * part + 256]).astype(bf16)
        y_ref[384 * part : 384 * part + 384, 768:1024] = r

    for half in range(2):
        rows = pl.ds(384 * half, 384)
        lhs = fwd_ref[rows, :]

        def part(n):
            return dot(lhs, y_ref[:, 256 * n : 256 * n + 256]) * gains_ref[:, 256 * n : 256 * n + 256]

        d = part(0)
        t_ref[:, 0:256] = d
        d = part(1)
        t_ref[:, 256:384] = d[:, 0:128]
        t_ref[:, 0:128] += d[:, 128:256]
        d = part(2)
        t_ref[:, 128:384] += d
        d = part(3)
        s_ref[rows, 0:128] = (t_ref[:, 0:128] + pltpu.roll(t_ref[:, 128:256], 64, 1) + d[:, 0:128]).astype(bf16)
        s_ref[rows, 128:256] = (t_ref[:, 256:384] + d[:, 128:256]).astype(bf16)

    mid_real = dot(inv_ref[0:384, :], s_ref[...]).astype(bf16)
    mid_imag = dot(inv_ref[384:768, :], s_ref[...]).astype(bf16)
    picture = dot(mid_real, out_w_ref[0:256, :]) + dot(mid_imag, out_w_ref[256:512, :])
    row_last = last_ref[slot, 0]
    col_last = last_ref[slot, 1]
    row_ramp = rows_ref[:, 0:1] * jnp.where(row_last > 0, 1.0, rows_ref[:, 1:2])
    col_ramp = cols_ref[0:1, :] * jnp.where(col_last > 0, 1.0, cols_ref[1:2, :])
    weighted = picture * row_ramp * col_ramp
    for chunk in range(16):
        out_ref[chunk, 0] = weighted[CHUNK * chunk : CHUNK * chunk + CHUNK, :].astype(bf16)


def ramps():
    places = np.arange(SIDE) + 0.5
    rising = np.minimum(places / OVERLAP, 1.0)
    falling = np.minimum((SIDE - places) / OVERLAP, 1.0)
    return rising, falling


def tile_results(frames, masks, phases, last, gains):
    slots = frames.shape[0]
    f32 = jnp.float32
    spread = jnp.repeat(masks.astype(f32), SIDE // masks.shape[2], axis=2)
    orders = np.arange(1, 3)
    angle = (np.outer(np.arange(SIDE), orders * SHIFT_ROWS) % SIDE) * (2 * math.pi / SIDE)
    row_c = jnp.asarray(np.cos(angle) / PHASES, f32)[None]
    row_s = jnp.asarray(np.sin(angle) / PHASES, f32)[None]
    turn = phases * jnp.asarray(orders, f32)[None]
    c, s = jnp.cos(turn)[:, None], jnp.sin(turn)[:, None]
    turns = jnp.stack([c * row_c - s * row_s, s * row_c + c * row_s], axis=3).reshape(slots, SIDE, 4)
    rising, falling = ramps()
    rows = jnp.asarray(np.stack([rising / (SIDE * SIDE), falling], axis=1), f32)
    cols = jnp.asarray(np.stack([rising, falling]), f32)
    tables = [
        table(first_table(1)), table(first_table(2)),
        table(centre_table()),
        table(forward_rows()), table(inverse_rows()), table(last_table()),
    ]

    def whole(array):
        return pl.BlockSpec(array.shape, lambda i, *_: (0,) * array.ndim)

    fixed = [gains, rows, cols] + tables
    return pl.pallas_call(
        tile_kernel,
        out_shape=jax.ShapeDtypeStruct((16, slots, CHUNK, SIDE), jnp.bfloat16),
        grid_spec=pltpu.PrefetchScalarGridSpec(
            num_scalar_prefetch=1,
            grid=(slots,),
            in_specs=[
                pl.BlockSpec((1, PHASES, SIDE, SIDE), lambda i, *_: (i, 0, 0, 0)),
                pl.BlockSpec((1, 12, SIDE), lambda i, *_: (i, 0, 0)),
                pl.BlockSpec((1, SIDE, 4), lambda i, *_: (i, 0, 0)),
            ] + [whole(one) for one in fixed],
            out_specs=pl.BlockSpec((16, 1, CHUNK, SIDE), lambda i, *_: (0, i, 0, 0)),
            scratch_shapes=[
                pltpu.VMEM((SIDE, 1920), jnp.bfloat16),
                pltpu.VMEM((2 * SIDE, 1024), jnp.bfloat16),
                pltpu.VMEM((SIDE, 384), jnp.float32),
                pltpu.VMEM((2 * SIDE, 256), jnp.bfloat16),
            ],
        ),
        cost_estimate=pl.CostEstimate(flops=slots * 3_000_000_000, bytes_accessed=12_000_000, transcendentals=0),
        name="tiles",
    )(last, frames, spread, turns, *fixed)


def pick_kernel(index_ref, in_ref, out_ref):
    def one(at, carry):
        source = index_ref[at]
        value = in_ref[jnp.maximum(source, 0)]
        out_ref[at] = jnp.where(source >= 0, value, jnp.zeros_like(value))
        return carry

    lax.fori_loop(0, out_ref.shape[0], one, 0, unroll=8)


def picked(groups, index):
    count = index.shape[0]
    return pl.pallas_call(
        pick_kernel,
        out_shape=jax.ShapeDtypeStruct((count,) + groups.shape[1:], groups.dtype),
        grid_spec=pltpu.PrefetchScalarGridSpec(
            num_scalar_prefetch=1,
            grid=(1,),
            in_specs=[pl.BlockSpec(groups.shape, lambda i, *_: (0, 0, 0))],
            out_specs=pl.BlockSpec((count,) + groups.shape[1:], lambda i, *_: (0, 0, 0)),
        ),
        name="pick",
    )(index, groups)


def shards(frames, masks, phases, slot_tile, otf, apod):
    devices = lax.axis_size("ty")
    group_count = lax.axis_size("tx")
    my_group = lax.axis_index("tx")
    me = lax.axis_index("ty")
    own = slot_tile[0]
    slots = own.shape[0]
    column = GROUP_COLS * my_group + own % GROUP_COLS
    last = jnp.stack(
        [own // GROUP_COLS == devices - 1, column == GROUP_COLS * group_count - 1], axis=1
    ).astype(jnp.int32)
    names = lax.all_to_all(jnp.broadcast_to(own[None], (devices, slots)), "ty", 0, 0, tiled=True)

    gains = band_gains(otf, apod)
    results = tile_results(frames[0, :, 0], masks[0], phases[0], last, gains)
    spread = lax.all_to_all(results, "ty", 0, 0, tiled=True)

    i = jnp.arange(CHUNK // GROUP, dtype=jnp.int32)
    ahead = ((CHUNK // GROUP) * me + i < OVERLAP // GROUP).astype(jnp.int32)
    rows = jnp.arange(devices, dtype=jnp.int32)[:, None, None] + ahead[None, None, :]
    wanted = GROUP_COLS * rows + jnp.arange(GROUP_COLS, dtype=jnp.int32)[None, :, None]
    flat = names.reshape(-1)
    hit = wanted[..., None] == flat
    place = jnp.sum(hit * jnp.arange(flat.shape[0], dtype=jnp.int32), axis=-1)
    index = jnp.where(rows < devices, place * (CHUNK // GROUP) + i, -1).reshape(-1)

    chosen = picked(spread.reshape(-1, GROUP, SIDE), index)
    home = lax.all_to_all(chosen.reshape(devices, GROUP_COLS * CHUNK, SIDE), "ty", 0, 0, tiled=True)

    tiles = home.reshape(devices, GROUP_COLS, CHUNK, SIDE).swapaxes(0, 1).reshape(GROUP_COLS, SIDE, SIDE)
    tiles = tiles.astype(jnp.float32)
    body = tiles[:, OVERLAP:]
    folded = jnp.concatenate(
        [body[:, : STRIDE - OVERLAP], body[:, STRIDE - OVERLAP :] + tiles[:, :OVERLAP]], axis=1
    )
    left, right = folded[0], folded[1]
    strip = lax.ppermute(
        left[:, :OVERLAP].astype(jnp.bfloat16), "tx", [(g, g - 1) for g in range(1, group_count)]
    ).astype(jnp.float32)
    joined = left[:, STRIDE:] + right[:, :OVERLAP]
    edge = right[:, STRIDE:] + strip
    return jnp.concatenate([left[:, OVERLAP:STRIDE], joined, right[:, OVERLAP:STRIDE], edge], axis=1)


def solution(mesh):
    in_specs = (
        P("tx", "ty", None, None, None, None),
        P("tx", "ty", None, None),
        P("tx", "ty", None),
        P("tx", "ty"),
        P(),
        P(),
    )
    return jax.shard_map(
        shards, mesh=mesh, in_specs=in_specs, out_specs=P("ty", "tx"), check_vma=False
    )
```

```python
import functools
import math

import jax
import jax.numpy as jnp
import numpy as np
from jax import lax
from jax.experimental import pallas as pl
from jax.experimental.pallas import tpu as pltpu
from jax.sharding import PartitionSpec as P

SIDE = 384
STRIDE = 320
OVERLAP = SIDE - STRIDE
GROUP_COLS = 2
PHASES = 5
CELLS = 12
WIENER = 0.1
SHIFT_ROWS, SHIFT_COLS = 37, 101
CHUNK = SIDE // 16
GROUP = 8
ROW_GROUPS = CHUNK // GROUP
TILE_GROUPS = 3 * ROW_GROUPS

COL_A = np.arange(64, 128)
COL_B = np.arange(128, 192)
COL_C = np.arange(0, 64)
NYQUIST = SIDE // 2


def cos_sin(rows, cols):
    angle = (np.outer(rows, cols) % SIDE) * (2.0 * math.pi / SIDE)
    return np.cos(angle), np.sin(angle)


def band_columns(order):
    move = order * SHIFT_COLS
    return np.concatenate([
        COL_B + move, COL_A + move, COL_B - move, COL_A - move,
        COL_C + move, [NYQUIST + move], COL_C[1:] - move,
    ])


def centre_table():
    cols = np.concatenate([COL_B, COL_A, COL_C, [NYQUIST]])
    c, s = cos_sin(np.arange(SIDE), cols)
    pad = np.zeros((SIDE, 63))
    return np.concatenate([c, pad, -s, pad], axis=1)


def last_table():
    lines = np.concatenate([COL_B, COL_A, COL_C, [NYQUIST], COL_C[1:]])
    c, s = cos_sin(lines, np.arange(SIDE))
    return np.concatenate([c, s], axis=0)


def table(values):
    return jnp.asarray(values.astype(np.float32)).astype(jnp.bfloat16)


def dot(x, w):
    return jnp.dot(x, w, preferred_element_type=jnp.float32)


def halves(x):
    high = x.astype(jnp.bfloat16)
    return high, (x - high.astype(jnp.float32)).astype(jnp.bfloat16)


def negated(x, flip):
    high, low = halves(x)
    high = dot(flip, high).astype(jnp.bfloat16)
    low = dot(flip, low).astype(jnp.bfloat16)
    return dot(high, flip) + dot(low, flip)


def fill_gains(otf_ref, apod_ref, work_ref, gains_ref):
    rows = lax.broadcasted_iota(jnp.int32, (SIDE, SIDE), 0)
    cols = lax.broadcasted_iota(jnp.int32, (SIDE, SIDE), 1)
    total = rows + cols
    flip = ((total == 0) | (total == SIDE)).astype(jnp.float32).astype(jnp.bfloat16)
    orders = range(-2, 3)

    def moved(source, order):
        if order:
            source = pltpu.roll(source, (-order * SHIFT_COLS) % SIDE, 1)[:, 0:256]
            return pltpu.roll(source, (-order * SHIFT_ROWS) % SIDE, 0)
        return source[:, 0:256]

    def fill(source, numerator, first):
        power = None
        for at, order in enumerate(orders):
            one = moved(source, order)
            work_ref[at] = one
            power = one * one if power is None else power + one * one
        scale = numerator / (WIENER + power)
        for at in range(5):
            at_rows = pl.ds(SIDE * at, SIDE)
            if first:
                gains_ref[at_rows, :] = work_ref[at] * scale
            else:
                gains_ref[at_rows, :] += work_ref[at] * scale

    fill(otf_ref[...], apod_ref[:, 0:256], True)
    fill(negated(otf_ref[...], flip), negated(apod_ref[...], flip)[:, 0:256], False)


def pack_gains(natural_ref, gains_ref):
    lane = lax.broadcasted_iota(jnp.int32, (SIDE, 128), 1)
    low = lane < 64
    nyquist = lane == 64

    def tiles(order):
        at = pl.ds(SIDE * (order + 2), SIDE)
        return natural_ref[at, 0:128], natural_ref[at, 128:256]

    for order in (1, 2):
        base = 256 * (order - 1)
        up0, up1 = tiles(order)
        down0, down1 = tiles(-order)
        gains_ref[:, base : base + 128] = jnp.where(low, up1, up0)
        gains_ref[:, base + 128 : base + 256] = jnp.where(low, down1, down0)
        rest = jnp.where(low, up0, jnp.where(nyquist, up1, pltpu.roll(down0, 64, 1)))
        gains_ref[:, 384 + 128 * order : 512 + 128 * order] = rest
    mid0, mid1 = tiles(0)
    gains_ref[:, 768:896] = jnp.where(low, mid1, mid0)
    edge = jnp.where(lane == 0, 0.5 * mid0, mid0)
    gains_ref[:, 896:1024] = jnp.where(low, edge, jnp.where(nyquist, 0.5 * mid1, 0.0))


def fill_tables(cos_ref, sin_ref, band_refs, weight_refs, fwd_ref):
    zero = jnp.zeros((), jnp.bfloat16)
    fwd_ref[0:384, 0:384] = cos_ref[...]
    fwd_ref[0:384, 384:768] = sin_ref[...]
    fwd_ref[384:768, 0:384] = zero - sin_ref[...]
    fwd_ref[384:768, 384:768] = cos_ref[...]
    upper = lax.broadcasted_iota(jnp.int32, (SIDE, 128), 1) < 65
    for (c_ref, s_ref), w_ref in zip(band_refs, weight_refs):
        w_ref[0:384, 0:384] = c_ref[...]
        w_ref[0:384, 384:768] = zero - s_ref[...]
        for tile in range(3):
            lanes = pl.ds(128 * tile, 128)
            c, s = c_ref[:, lanes], s_ref[:, lanes]
            if tile == 0:
                c, s = zero - c, zero - s
            elif tile == 2:
                c = jnp.where(upper, -c.astype(jnp.float32), c.astype(jnp.float32)).astype(jnp.bfloat16)
                s = jnp.where(upper, -s.astype(jnp.float32), s.astype(jnp.float32)).astype(jnp.bfloat16)
            w_ref[384:768, lanes] = s
            w_ref[384:768, pl.ds(384 + 128 * tile, 128)] = c


def tile_kernel(
    devices, group_count,
    names_ref, phases_ref,
    frames_hbm, masks_ref, otf_hbm, apod_hbm, rows_ref, cols_ref,
    cos_hbm, sin_hbm, c1_hbm, s1_hbm, c2_hbm, s2_hbm, w0_hbm, last_hbm,
    out_ref,
    frames_ref, otf_ref, apod_ref, cos_ref, sin_ref, c1_ref, s1_ref, c2_ref, s2_ref, w0_ref, last_ref,
    work_ref, natural_ref, gains_ref, w1_ref, w2_ref, fwd_ref, left_ref, y_ref, s_ref, t_ref, sems,
):
    slot = pl.program_id(0)
    f32, bf16 = jnp.float32, jnp.bfloat16
    k1, k2 = math.cos(2 * math.pi / 5), math.cos(4 * math.pi / 5)
    n1, n2 = math.sin(2 * math.pi / 5), math.sin(4 * math.pi / 5)
    slots = frames_ref.shape[0]

    fixed = [
        (otf_hbm, otf_ref), (apod_hbm, apod_ref), (cos_hbm, cos_ref), (sin_hbm, sin_ref),
        (c1_hbm, c1_ref), (s1_hbm, s1_ref), (c2_hbm, c2_ref), (s2_hbm, s2_ref),
        (w0_hbm, w0_ref), (last_hbm, last_ref),
    ]

    def fixed_copy(at):
        return pltpu.make_async_copy(fixed[at][0], fixed[at][1], sems.at[at])

    def frame_copy(at):
        return pltpu.make_async_copy(frames_hbm.at[at], frames_ref.at[at], sems.at[len(fixed) + at])

    @pl.when(slot == 0)
    def _():
        for at in range(len(fixed)):
            fixed_copy(at).start()
        for at in range(slots):
            frame_copy(at).start()
        line = lax.broadcasted_iota(jnp.int32, (GROUP, 128), 0)
        tags = jnp.full((GROUP, 128), -1.0, f32)
        for at in range(slots):
            tags = jnp.where(line == at, names_ref[0, at].astype(f32), tags)
        for chunk in range(devices):
            out_ref[chunk, TILE_GROUPS * slots] = tags.astype(bf16)
        fixed_copy(0).wait()
        fixed_copy(1).wait()
        fill_gains(otf_ref, apod_ref, work_ref, natural_ref)
        pack_gains(natural_ref, gains_ref)
        for at in range(2, len(fixed)):
            fixed_copy(at).wait()
        fill_tables(cos_ref, sin_ref, ((c1_ref, s1_ref), (c2_ref, s2_ref)), (w1_ref, w2_ref), fwd_ref)

    for at in range(slots):
        @pl.when(slot == at)
        def _():
            frame_copy(at).wait()

    cell_row = lax.broadcasted_iota(jnp.int32, (CELLS, SIDE), 0)
    cell_col = lax.broadcasted_iota(jnp.int32, (CELLS, SIDE), 1) // (SIDE // CELLS)
    spread = (cell_row == cell_col).astype(f32).astype(bf16)
    flags = dot(masks_ref[0].astype(f32).astype(bf16), spread)

    phase = jnp.full((GROUP, 128), phases_ref[slot, 0], f32)
    turns = [[fn(order * phase)[0:1, 0:1] for fn in (jnp.cos, jnp.sin)] for order in (1.0, 2.0)]

    for cell in range(CELLS):
        rows = pl.ds(32 * cell, 32)
        flag = flags[cell : cell + 1, :]
        f = [frames_ref[slot, p, rows, :].astype(f32) * flag for p in range(PHASES)]
        a1, d1, a2, d2 = f[1] + f[4], f[1] - f[4], f[2] + f[3], f[2] - f[3]
        left_ref[rows, 1536:1920] = ((f[0] + a1 + a2) * (1.0 / PHASES)).astype(bf16)
        for at, (a, b) in enumerate((
            (f[0] + k1 * a1 + k2 * a2, n1 * d1 + n2 * d2),
            (f[0] + k2 * a1 + k1 * a2, n2 * d1 - n1 * d2),
        )):
            turn_c, turn_s = turns[at]
            row_c, row_s = rows_ref[rows, 2 + 2 * at : 3 + 2 * at], rows_ref[rows, 3 + 2 * at : 4 + 2 * at]
            c = turn_c * row_c - turn_s * row_s
            s = turn_s * row_c + turn_c * row_s
            left_ref[rows, 768 * at : 768 * at + 384] = (c * a - s * b).astype(bf16)
            left_ref[rows, 768 * at + 384 : 768 * at + 768] = (c * b + s * a).astype(bf16)

    for at, w_ref in enumerate((w1_ref, w2_ref)):
        columns = (256 * at, 256 * at + 128, 512 + 128 * at)
        for part in range(3):
            r = dot(left_ref[:, 768 * at : 768 * at + 768], w_ref[:, 256 * part : 256 * part + 256]).astype(bf16)
            for half in range(2):
                tile = 2 * part + half
                base = 384 if tile >= 3 else 0
                col = columns[tile % 3]
                y_ref[base : base + 384, col : col + 128] = r[:, 128 * half : 128 * half + 128]
    for part in range(2):
        r = dot(left_ref[:, 1536:1920], w0_ref[:, 256 * part : 256 * part + 256]).astype(bf16)
        y_ref[384 * part : 384 * part + 384, 768:1024] = r

    for half in range(2):
        rows = pl.ds(384 * half, 384)
        lhs = fwd_ref[rows, :]
        sign = 1.0 - 2.0 * half

        def part(n):
            lanes = pl.ds(256 * n, 256)
            return dot(lhs, y_ref[:, lanes]) * gains_ref[:, lanes]

        d = part(0)
        t_ref[:, 0:128] = d[:, 0:128] + d[:, 128:256]
        d = part(1)
        t_ref[:, 0:128] += d[:, 0:128] + d[:, 128:256]
        d = part(2)
        t_ref[:, 128:256] = d[:, 0:128] + d[:, 128:256]
        d = part(3)
        s_ref[rows, :] = (sign * (t_ref[...] + d)).astype(bf16)

    mid_real = dot(fwd_ref[0:384, :], s_ref[...]).astype(bf16)
    mid_imag = dot(fwd_ref[384:768, :], s_ref[...]).astype(bf16)
    picture = dot(mid_real, last_ref[0:256, :]) + dot(mid_imag, last_ref[256:512, :])
    name = names_ref[0, slot]
    row_last = name >= GROUP_COLS * (devices - 1)
    col_last = (lax.axis_index("tx") == group_count - 1) & (lax.rem(name, GROUP_COLS) == GROUP_COLS - 1)
    row_ramp = rows_ref[:, 0:1] * jnp.where(row_last, 1.0, rows_ref[:, 1:2])
    col_ramp = cols_ref[0:1, :] * jnp.where(col_last, 1.0, cols_ref[1:2, :])
    weighted = picture * row_ramp * col_ramp
    for part in range(SIDE // GROUP):
        chunk, i = part // ROW_GROUPS, part % ROW_GROUPS
        for tile in range(3):
            piece = weighted[GROUP * part : GROUP * part + GROUP, 128 * tile : 128 * tile + 128]
            out_ref[chunk, TILE_GROUPS * slot + ROW_GROUPS * tile + i] = piece.astype(bf16)


def row_constants():
    places = np.arange(SIDE) + 0.5
    rising = np.minimum(places / OVERLAP, 1.0)
    falling = np.minimum((SIDE - places) / OVERLAP, 1.0)
    columns = [rising / (SIDE * SIDE), falling]
    for order in (1, 2):
        angle = (np.arange(SIDE) * order * SHIFT_ROWS % SIDE) * (2 * math.pi / SIDE)
        columns += [np.cos(angle) / PHASES, np.sin(angle) / PHASES]
    return np.stack(columns, axis=1), np.stack([rising, falling])


def tile_results(frames, masks, phases, names, otf, apod, devices, group_count):
    slots = frames.shape[0]
    f32, bf16 = jnp.float32, jnp.bfloat16
    rows, cols = (jnp.asarray(one, f32) for one in row_constants())
    every = np.arange(SIDE)
    tables = [*cos_sin(every, every), *cos_sin(every, band_columns(1)), *cos_sin(every, band_columns(2))]
    tables = [table(one) for one in tables + [centre_table(), last_table()]]
    places = pl.BlockSpec(memory_space=pl.ANY)

    def whole(array):
        return pl.BlockSpec(array.shape, lambda i, *_: (0,) * array.ndim)

    def like(array):
        return pltpu.VMEM(array.shape, array.dtype)

    return pl.pallas_call(
        functools.partial(tile_kernel, devices, group_count),
        out_shape=jax.ShapeDtypeStruct((devices, TILE_GROUPS * slots + 1, GROUP, 128), bf16),
        grid_spec=pltpu.PrefetchScalarGridSpec(
            num_scalar_prefetch=2,
            grid=(slots,),
            in_specs=[
                places,
                pl.BlockSpec((1, CELLS, CELLS), lambda i, *_: (i, 0, 0)),
                places, places, whole(rows), whole(cols),
            ] + [places] * len(tables),
            out_specs=pl.BlockSpec(memory_space=pltpu.VMEM),
            scratch_shapes=[like(frames), like(otf), like(apod)] + [like(one) for one in tables] + [
                pltpu.VMEM((5, SIDE, 256), f32),
                pltpu.VMEM((5 * SIDE, 256), f32),
                pltpu.VMEM((SIDE, 1024), f32),
                pltpu.VMEM((2 * SIDE, 2 * SIDE), bf16),
                pltpu.VMEM((2 * SIDE, 2 * SIDE), bf16),
                pltpu.VMEM((2 * SIDE, 2 * SIDE), bf16),
                pltpu.VMEM((SIDE, 1920), bf16),
                pltpu.VMEM((2 * SIDE, 1024), bf16),
                pltpu.VMEM((2 * SIDE, 256), bf16),
                pltpu.VMEM((SIDE, 256), f32),
                pltpu.SemaphoreType.DMA((2 + len(tables) + slots,)),
            ],
        ),
        cost_estimate=pl.CostEstimate(flops=slots * 3_000_000_000, bytes_accessed=12_000_000, transcendentals=0),
        name="tiles",
    )(names, phases, frames, masks, otf, apod, rows, cols, *tables)


def pick_kernel(slots, devices, in_ref, out_ref, where_ref, place_ref, sem):
    me = lax.axis_index("ty")
    per_device = TILE_GROUPS * slots + 1
    line = lax.broadcasted_iota(jnp.int32, (GROUP, 128), 0)
    lane = lax.broadcasted_iota(jnp.int32, (GROUP, 128), 1).astype(jnp.float32)
    place = jnp.zeros((GROUP, 128), jnp.int32)
    for source in range(devices):
        tags = in_ref[source, per_device - 1].astype(jnp.float32)
        place += jnp.where(tags == lane, per_device * source + TILE_GROUPS * line, 0)
    where_ref[...] = jnp.sum(place, axis=0, keepdims=True)
    copy = pltpu.make_async_copy(where_ref, place_ref, sem)
    copy.start()
    copy.wait()

    for i in range(ROW_GROUPS):
        ahead = (ROW_GROUPS * me + i < OVERLAP // GROUP).astype(jnp.int32)
        for target in range(devices):
            row = target + ahead
            held = row < devices
            for col in range(GROUP_COLS):
                source = place_ref[0, GROUP_COLS * row + col]
                home = source // per_device
                group = source - per_device * home
                for tile in range(3):
                    value = in_ref[home, group + ROW_GROUPS * tile + i]
                    if target == devices - 1:
                        value = jnp.where(held, value, jnp.zeros_like(value))
                    out_ref[target, TILE_GROUPS * col + ROW_GROUPS * tile + i] = value


def picked(spread, slots):
    devices = spread.shape[0]
    return pl.pallas_call(
        functools.partial(pick_kernel, slots, devices),
        out_shape=jax.ShapeDtypeStruct((devices, GROUP_COLS * TILE_GROUPS, GROUP, 128), spread.dtype),
        in_specs=[pl.BlockSpec(memory_space=pltpu.VMEM)],
        out_specs=pl.BlockSpec(memory_space=pltpu.VMEM),
        scratch_shapes=[
            pltpu.VMEM((1, 128), jnp.int32), pltpu.SMEM((1, 128), jnp.int32), pltpu.SemaphoreType.DMA,
        ],
        name="pick",
    )(spread)


def folded(in_ref, col, tile):
    rows = []
    for part in range(SIDE // GROUP):
        value = in_ref[part // ROW_GROUPS, TILE_GROUPS * col + ROW_GROUPS * tile + part % ROW_GROUPS]
        rows.append(value.astype(jnp.float32))
    count = OVERLAP // GROUP
    body = rows[count:]
    for at in range(count):
        body[len(body) - count + at] = body[len(body) - count + at] + rows[at]
    return jnp.concatenate(body, axis=0)


def strip_kernel(in_ref, out_ref):
    out_ref[...] = folded(in_ref, 0, 0).astype(jnp.bfloat16)


def join_kernel(in_ref, strip_ref, out_ref):
    low = lax.broadcasted_iota(jnp.int32, (STRIDE, 128), 1) < OVERLAP
    left = [pltpu.roll(folded(in_ref, 0, tile), OVERLAP, 1) for tile in range(3)]
    right = [folded(in_ref, 1, tile) for tile in range(3)]
    out_ref[:, 0:128] = jnp.where(low, left[0], left[1])
    out_ref[:, 128:256] = jnp.where(low, left[1], left[2])
    out_ref[:, 256:384] = right[0] + jnp.where(low, left[2], 0.0)
    out_ref[:, 384:512] = right[1]
    strip = pltpu.roll(strip_ref[...].astype(jnp.float32), OVERLAP, 1)
    out_ref[:, 512:640] = right[2] + jnp.where(low, 0.0, strip)


def shards(frames, masks, phases, slot_tile, otf, apod):
    devices = lax.axis_size("ty")
    group_count = lax.axis_size("tx")
    slots = frames.shape[1]
    results = tile_results(
        frames[0, :, 0], masks[0], phases[0], slot_tile, otf, apod, devices, group_count
    )
    spread = lax.all_to_all(results, "ty", 0, 0, tiled=True)
    home = lax.all_to_all(picked(spread, slots), "ty", 0, 0, tiled=True)
    in_vmem = pl.BlockSpec(memory_space=pltpu.VMEM)
    strip = pl.pallas_call(
        strip_kernel,
        out_shape=jax.ShapeDtypeStruct((STRIDE, 128), jnp.bfloat16),
        in_specs=[in_vmem], out_specs=in_vmem, name="strip",
    )(home)
    strip = lax.ppermute(strip, "tx", [(g, g - 1) for g in range(1, group_count)])
    return pl.pallas_call(
        join_kernel,
        out_shape=jax.ShapeDtypeStruct((STRIDE, STRIDE * GROUP_COLS), jnp.float32),
        in_specs=[in_vmem, in_vmem], out_specs=in_vmem, name="join",
    )(home, strip)


def solution(mesh):
    in_specs = (
        P("tx", "ty", None, None, None, None),
        P("tx", "ty", None, None),
        P("tx", "ty", None),
        P("tx", "ty"),
        P(),
        P(),
    )
    return jax.shard_map(
        shards, mesh=mesh, in_specs=in_specs, out_specs=P("ty", "tx"), check_vma=False
    )
```

```python
import functools
import math

import jax
import jax.numpy as jnp
import numpy as np
from jax import lax
from jax.experimental import pallas as pl
from jax.experimental.pallas import tpu as pltpu
from jax.sharding import PartitionSpec as P

SIDE = 384
STRIDE = 320
OVERLAP = SIDE - STRIDE
GROUP_COLS = 2
PHASES = 5
CELLS = 12
WIENER = 0.1
SHIFT_ROWS, SHIFT_COLS = 37, 101
CHUNK = SIDE // 16
SMALL_VMEM = 4 << 20
GROUP = 8
ROW_GROUPS = CHUNK // GROUP
TILE_GROUPS = 3 * ROW_GROUPS

COL_A = np.arange(64, 128)
COL_B = np.arange(128, 192)
COL_C = np.arange(0, 64)
NYQUIST = SIDE // 2


def cos_sin(rows, cols):
    angle = (np.outer(rows, cols) % SIDE) * (2.0 * math.pi / SIDE)
    return np.cos(angle), np.sin(angle)


def band_columns(order):
    move = order * SHIFT_COLS
    return np.concatenate([
        COL_B + move, COL_A + move, COL_B - move, COL_A - move,
        COL_C + move, [NYQUIST + move], COL_C[1:] - move,
    ])


def centre_table():
    cols = np.concatenate([COL_B, COL_A, COL_C, [NYQUIST]])
    c, s = cos_sin(np.arange(SIDE), cols)
    pad = np.zeros((SIDE, 63))
    return np.concatenate([c, pad, -s, pad], axis=1)


def last_table():
    lines = np.concatenate([COL_B, COL_A, COL_C, [NYQUIST], COL_C[1:]])
    c, s = cos_sin(lines, np.arange(SIDE))
    return np.concatenate([c, s], axis=0)


def table(values):
    return jnp.asarray(values.astype(np.float32)).astype(jnp.bfloat16)


def dot(x, w):
    return jnp.dot(x, w, preferred_element_type=jnp.float32)


def halves(x):
    high = x.astype(jnp.bfloat16)
    return high, (x - high.astype(jnp.float32)).astype(jnp.bfloat16)


def negated(x, flip):
    high, low = halves(x)
    high = dot(flip, high).astype(jnp.bfloat16)
    low = dot(flip, low).astype(jnp.bfloat16)
    return dot(high, flip) + dot(low, flip)


def fill_gains(otf_ref, apod_ref, work_ref, gains_ref):
    rows = lax.broadcasted_iota(jnp.int32, (SIDE, SIDE), 0)
    cols = lax.broadcasted_iota(jnp.int32, (SIDE, SIDE), 1)
    total = rows + cols
    flip = ((total == 0) | (total == SIDE)).astype(jnp.float32).astype(jnp.bfloat16)
    orders = range(-2, 3)

    def moved(source, order):
        if order:
            source = pltpu.roll(source, (-order * SHIFT_COLS) % SIDE, 1)[:, 0:256]
            return pltpu.roll(source, (-order * SHIFT_ROWS) % SIDE, 0)
        return source[:, 0:256]

    def fill(source, numerator, first):
        power = None
        for at, order in enumerate(orders):
            one = moved(source, order)
            work_ref[at] = one
            power = one * one if power is None else power + one * one
        scale = numerator / (WIENER + power)
        for at in range(5):
            at_rows = pl.ds(SIDE * at, SIDE)
            if first:
                gains_ref[at_rows, :] = work_ref[at] * scale
            else:
                gains_ref[at_rows, :] += work_ref[at] * scale

    fill(otf_ref[...], apod_ref[:, 0:256], True)
    fill(negated(otf_ref[...], flip), negated(apod_ref[...], flip)[:, 0:256], False)


def pack_gains(natural_ref, gains_ref):
    lane = lax.broadcasted_iota(jnp.int32, (SIDE, 128), 1)
    low = lane < 64
    nyquist = lane == 64

    def tiles(order):
        at = pl.ds(SIDE * (order + 2), SIDE)
        return natural_ref[at, 0:128], natural_ref[at, 128:256]

    for order in (1, 2):
        base = 256 * (order - 1)
        up0, up1 = tiles(order)
        down0, down1 = tiles(-order)
        gains_ref[:, base : base + 128] = jnp.where(low, up1, up0)
        gains_ref[:, base + 128 : base + 256] = jnp.where(low, down1, down0)
        rest = jnp.where(low, up0, jnp.where(nyquist, up1, pltpu.roll(down0, 64, 1)))
        gains_ref[:, 384 + 128 * order : 512 + 128 * order] = rest
    mid0, mid1 = tiles(0)
    gains_ref[:, 768:896] = jnp.where(low, mid1, mid0)
    edge = jnp.where(lane == 0, 0.5 * mid0, mid0)
    gains_ref[:, 896:1024] = jnp.where(low, edge, jnp.where(nyquist, 0.5 * mid1, 0.0))


def fill_tables(cos_ref, sin_ref, band_refs, weight_refs, fwd_ref):
    zero = jnp.zeros((), jnp.bfloat16)
    fwd_ref[0:384, 0:384] = cos_ref[...]
    fwd_ref[0:384, 384:768] = sin_ref[...]
    fwd_ref[384:768, 0:384] = zero - sin_ref[...]
    fwd_ref[384:768, 384:768] = cos_ref[...]
    upper = lax.broadcasted_iota(jnp.int32, (SIDE, 128), 1) < 65
    for (c_ref, s_ref), w_ref in zip(band_refs, weight_refs):
        w_ref[0:384, 0:384] = c_ref[...]
        w_ref[0:384, 384:768] = zero - s_ref[...]
        for tile in range(3):
            lanes = pl.ds(128 * tile, 128)
            c, s = c_ref[:, lanes], s_ref[:, lanes]
            if tile == 0:
                c, s = zero - c, zero - s
            elif tile == 2:
                c = jnp.where(upper, -c.astype(jnp.float32), c.astype(jnp.float32)).astype(jnp.bfloat16)
                s = jnp.where(upper, -s.astype(jnp.float32), s.astype(jnp.float32)).astype(jnp.bfloat16)
            w_ref[384:768, lanes] = s
            w_ref[384:768, pl.ds(384 + 128 * tile, 128)] = c


def tile_kernel(
    devices, group_count,
    names_ref, phases_ref,
    frames_hbm, masks_ref, otf_hbm, apod_hbm, rows_ref, cols_ref,
    cos_hbm, sin_hbm, c1_hbm, s1_hbm, c2_hbm, s2_hbm, w0_hbm, last_hbm,
    out_ref,
    frames_ref, otf_ref, apod_ref, cos_ref, sin_ref, c1_ref, s1_ref, c2_ref, s2_ref, w0_ref, last_ref,
    work_ref, natural_ref, gains_ref, w1_ref, w2_ref, fwd_ref, left_ref, y_ref, s_ref, t_ref, sems,
):
    slot = pl.program_id(0)
    f32, bf16 = jnp.float32, jnp.bfloat16
    k1, k2 = math.cos(2 * math.pi / 5), math.cos(4 * math.pi / 5)
    n1, n2 = math.sin(2 * math.pi / 5), math.sin(4 * math.pi / 5)
    slots = frames_ref.shape[0]

    fixed = [
        (otf_hbm, otf_ref), (apod_hbm, apod_ref), (cos_hbm, cos_ref), (sin_hbm, sin_ref),
        (c1_hbm, c1_ref), (s1_hbm, s1_ref), (c2_hbm, c2_ref), (s2_hbm, s2_ref),
        (w0_hbm, w0_ref), (last_hbm, last_ref),
    ]

    def fixed_copy(at):
        return pltpu.make_async_copy(fixed[at][0], fixed[at][1], sems.at[at])

    def frame_copy(at):
        return pltpu.make_async_copy(frames_hbm.at[at], frames_ref.at[at], sems.at[len(fixed) + at])

    @pl.when(slot == 0)
    def _():
        for at in range(len(fixed)):
            fixed_copy(at).start()
        for at in range(slots):
            frame_copy(at).start()
        line = lax.broadcasted_iota(jnp.int32, (GROUP, 128), 0)
        tags = jnp.full((GROUP, 128), -1.0, f32)
        for at in range(slots):
            tags = jnp.where(line == at, names_ref[0, at].astype(f32), tags)
        for chunk in range(devices):
            out_ref[chunk, TILE_GROUPS * slots] = tags.astype(bf16)
        fixed_copy(0).wait()
        fixed_copy(1).wait()
        fill_gains(otf_ref, apod_ref, work_ref, natural_ref)
        pack_gains(natural_ref, gains_ref)
        for at in range(2, len(fixed)):
            fixed_copy(at).wait()
        fill_tables(cos_ref, sin_ref, ((c1_ref, s1_ref), (c2_ref, s2_ref)), (w1_ref, w2_ref), fwd_ref)

    for at in range(slots):
        @pl.when(slot == at)
        def _():
            frame_copy(at).wait()

    cell_row = lax.broadcasted_iota(jnp.int32, (CELLS, SIDE), 0)
    cell_col = lax.broadcasted_iota(jnp.int32, (CELLS, SIDE), 1) // (SIDE // CELLS)
    spread = (cell_row == cell_col).astype(f32).astype(bf16)
    held = jnp.concatenate([masks_ref[0, row] for row in range(CELLS)], axis=0)
    flags = dot(held.astype(f32).astype(bf16), spread)

    phase = jnp.full((GROUP, 128), phases_ref[0, slot], f32)
    turns = [[fn(order * phase)[0:1, 0:1] for fn in (jnp.cos, jnp.sin)] for order in (1.0, 2.0)]

    for cell in range(CELLS):
        rows = pl.ds(32 * cell, 32)
        flag = flags[cell : cell + 1, :]
        f = [frames_ref[slot, p, rows, :].astype(f32) * flag for p in range(PHASES)]
        a1, d1, a2, d2 = f[1] + f[4], f[1] - f[4], f[2] + f[3], f[2] - f[3]
        left_ref[rows, 1536:1920] = ((f[0] + a1 + a2) * (1.0 / PHASES)).astype(bf16)
        for at, (a, b) in enumerate((
            (f[0] + k1 * a1 + k2 * a2, n1 * d1 + n2 * d2),
            (f[0] + k2 * a1 + k1 * a2, n2 * d1 - n1 * d2),
        )):
            turn_c, turn_s = turns[at]
            row_c, row_s = rows_ref[rows, 2 + 2 * at : 3 + 2 * at], rows_ref[rows, 3 + 2 * at : 4 + 2 * at]
            c = turn_c * row_c - turn_s * row_s
            s = turn_s * row_c + turn_c * row_s
            left_ref[rows, 768 * at : 768 * at + 384] = (c * a - s * b).astype(bf16)
            left_ref[rows, 768 * at + 384 : 768 * at + 768] = (c * b + s * a).astype(bf16)

    for at, w_ref in enumerate((w1_ref, w2_ref)):
        columns = (256 * at, 256 * at + 128, 512 + 128 * at)
        for part in range(3):
            r = dot(left_ref[:, 768 * at : 768 * at + 768], w_ref[:, 256 * part : 256 * part + 256]).astype(bf16)
            for half in range(2):
                tile = 2 * part + half
                base = 384 if tile >= 3 else 0
                col = columns[tile % 3]
                y_ref[base : base + 384, col : col + 128] = r[:, 128 * half : 128 * half + 128]
    for part in range(2):
        r = dot(left_ref[:, 1536:1920], w0_ref[:, 256 * part : 256 * part + 256]).astype(bf16)
        y_ref[384 * part : 384 * part + 384, 768:1024] = r

    for half in range(2):
        rows = pl.ds(384 * half, 384)
        lhs = fwd_ref[rows, :]
        sign = 1.0 - 2.0 * half

        def part(n):
            lanes = pl.ds(256 * n, 256)
            return dot(lhs, y_ref[:, lanes]) * gains_ref[:, lanes]

        d = part(0)
        t_ref[:, 0:128] = d[:, 0:128] + d[:, 128:256]
        d = part(1)
        t_ref[:, 0:128] += d[:, 0:128] + d[:, 128:256]
        d = part(2)
        t_ref[:, 128:256] = d[:, 0:128] + d[:, 128:256]
        d = part(3)
        s_ref[rows, :] = (sign * (t_ref[...] + d)).astype(bf16)

    mid_real = dot(fwd_ref[0:384, :], s_ref[...]).astype(bf16)
    mid_imag = dot(fwd_ref[384:768, :], s_ref[...]).astype(bf16)
    picture = dot(mid_real, last_ref[0:256, :]) + dot(mid_imag, last_ref[256:512, :])
    name = names_ref[0, slot]
    row_last = name >= GROUP_COLS * (devices - 1)
    col_last = (lax.axis_index("tx") == group_count - 1) & (lax.rem(name, GROUP_COLS) == GROUP_COLS - 1)
    row_ramp = rows_ref[:, 0:1] * jnp.where(row_last, 1.0, rows_ref[:, 1:2])
    col_ramp = cols_ref[0:1, :] * jnp.where(col_last, 1.0, cols_ref[1:2, :])
    weighted = picture * row_ramp * col_ramp
    for part in range(SIDE // GROUP):
        chunk, i = part // ROW_GROUPS, part % ROW_GROUPS
        for tile in range(3):
            piece = weighted[GROUP * part : GROUP * part + GROUP, 128 * tile : 128 * tile + 128]
            out_ref[chunk, TILE_GROUPS * slot + ROW_GROUPS * tile + i] = piece.astype(bf16)


def row_constants():
    places = np.arange(SIDE) + 0.5
    rising = np.minimum(places / OVERLAP, 1.0)
    falling = np.minimum((SIDE - places) / OVERLAP, 1.0)
    columns = [rising / (SIDE * SIDE), falling]
    for order in (1, 2):
        angle = (np.arange(SIDE) * order * SHIFT_ROWS % SIDE) * (2 * math.pi / SIDE)
        columns += [np.cos(angle) / PHASES, np.sin(angle) / PHASES]
    return np.stack(columns, axis=1), np.stack([rising, falling])


def tile_results(frames, masks, phases, names, otf, apod, devices, group_count):
    slots = frames.shape[0]
    f32, bf16 = jnp.float32, jnp.bfloat16
    rows, cols = (jnp.asarray(one, f32) for one in row_constants())
    every = np.arange(SIDE)
    tables = [*cos_sin(every, every), *cos_sin(every, band_columns(1)), *cos_sin(every, band_columns(2))]
    tables = [table(one) for one in tables + [centre_table(), last_table()]]
    places = pl.BlockSpec(memory_space=pl.ANY)

    def whole(array):
        return pl.BlockSpec(array.shape, lambda i, *_: (0,) * array.ndim)

    def like(array):
        return pltpu.VMEM(array.shape, array.dtype)

    return pl.pallas_call(
        functools.partial(tile_kernel, devices, group_count),
        out_shape=jax.ShapeDtypeStruct((devices, TILE_GROUPS * slots + 1, GROUP, 128), bf16),
        grid_spec=pltpu.PrefetchScalarGridSpec(
            num_scalar_prefetch=2,
            grid=(slots,),
            in_specs=[
                places,
                pl.BlockSpec((1, CELLS, 1, CELLS), lambda i, *_: (i, 0, 0, 0)),
                places, places, whole(rows), whole(cols),
            ] + [places] * len(tables),
            out_specs=pl.BlockSpec(memory_space=pltpu.VMEM),
            scratch_shapes=[like(frames), like(otf), like(apod)] + [like(one) for one in tables] + [
                pltpu.VMEM((5, SIDE, 256), f32),
                pltpu.VMEM((5 * SIDE, 256), f32),
                pltpu.VMEM((SIDE, 1024), f32),
                pltpu.VMEM((2 * SIDE, 2 * SIDE), bf16),
                pltpu.VMEM((2 * SIDE, 2 * SIDE), bf16),
                pltpu.VMEM((2 * SIDE, 2 * SIDE), bf16),
                pltpu.VMEM((SIDE, 1920), bf16),
                pltpu.VMEM((2 * SIDE, 1024), bf16),
                pltpu.VMEM((2 * SIDE, 256), bf16),
                pltpu.VMEM((SIDE, 256), f32),
                pltpu.SemaphoreType.DMA((2 + len(tables) + slots,)),
            ],
        ),
        cost_estimate=pl.CostEstimate(flops=slots * 3_000_000_000, bytes_accessed=12_000_000, transcendentals=0),
        name="tiles",
    )(names, phases, frames, masks, otf, apod, rows, cols, *tables)


def pick_kernel(slots, devices, in_ref, out_ref, where_ref, place_ref, sem):
    me = lax.axis_index("ty")
    per_device = TILE_GROUPS * slots + 1
    line = lax.broadcasted_iota(jnp.int32, (GROUP, 128), 0)
    lane = lax.broadcasted_iota(jnp.int32, (GROUP, 128), 1).astype(jnp.float32)
    place = jnp.zeros((GROUP, 128), jnp.int32)
    for source in range(devices):
        tags = in_ref[per_device * source + per_device - 1].astype(jnp.float32)
        place += jnp.where(tags == lane, per_device * source + TILE_GROUPS * line, 0)
    where_ref[...] = jnp.sum(place, axis=0, keepdims=True)
    copy = pltpu.make_async_copy(where_ref, place_ref, sem)
    copy.start()
    copy.wait()

    for i in range(ROW_GROUPS):
        ahead = (ROW_GROUPS * me + i < OVERLAP // GROUP).astype(jnp.int32)
        for target in range(devices):
            row = target + ahead
            for col in range(GROUP_COLS):
                source = place_ref[0, GROUP_COLS * row + col] + i
                for tile in range(3):
                    value = in_ref[source + ROW_GROUPS * tile]
                    if target == devices - 1:
                        value = jnp.where(row < devices, value, jnp.zeros_like(value))
                    out_ref[TILE_GROUPS * (GROUP_COLS * target + col) + ROW_GROUPS * tile + i] = value


def picked(spread, slots):
    devices = spread.shape[0]
    chosen = pl.pallas_call(
        functools.partial(pick_kernel, slots, devices),
        out_shape=jax.ShapeDtypeStruct((devices * GROUP_COLS * TILE_GROUPS, GROUP, 128), spread.dtype),
        in_specs=[pl.BlockSpec(memory_space=pltpu.VMEM)],
        out_specs=pl.BlockSpec(memory_space=pltpu.VMEM),
        scratch_shapes=[
            pltpu.VMEM((1, 128), jnp.int32), pltpu.SMEM((1, 128), jnp.int32), pltpu.SemaphoreType.DMA,
        ],
        compiler_params=pltpu.CompilerParams(vmem_limit_bytes=SMALL_VMEM),
        name="pick",
    )(spread.reshape(-1, GROUP, 128))
    return chosen.reshape(devices, -1, GROUP, 128)


def folded(in_ref, base):
    rows = []
    for part in range(SIDE // GROUP):
        value = in_ref[part // ROW_GROUPS, base + part % ROW_GROUPS]
        rows.append(value.astype(jnp.float32))
    count = OVERLAP // GROUP
    body = rows[count:]
    for at in range(count):
        body[len(body) - count + at] = body[len(body) - count + at] + rows[at]
    return jnp.concatenate(body, axis=0)


def join_kernel(in_ref, strip_ref, out_ref):
    low = lax.broadcasted_iota(jnp.int32, (STRIDE, 128), 1) < OVERLAP
    left = [pltpu.roll(folded(in_ref, ROW_GROUPS * tile), OVERLAP, 1) for tile in range(3)]
    right = [folded(in_ref, TILE_GROUPS + ROW_GROUPS * tile) for tile in range(3)]
    out_ref[:, 0:128] = jnp.where(low, left[0], left[1])
    out_ref[:, 128:256] = jnp.where(low, left[1], left[2])
    out_ref[:, 256:384] = right[0] + jnp.where(low, left[2], 0.0)
    out_ref[:, 384:512] = right[1]
    strip = pltpu.roll(folded(strip_ref, 0), OVERLAP, 1)
    out_ref[:, 512:640] = right[2] + jnp.where(low, 0.0, strip)


def shards(frames, masks, phases, slot_tile, otf, apod):
    devices = lax.axis_size("ty")
    group_count = lax.axis_size("tx")
    slots = frames.shape[1]
    results = tile_results(
        frames[0, :, 0], masks[0][:, :, None, :], phases[:, :, 0], slot_tile, otf, apod, devices, group_count
    )
    spread = lax.all_to_all(results, "ty", 0, 0, tiled=True)
    home = lax.all_to_all(picked(spread, slots), "ty", 0, 0, tiled=True)
    strip = lax.ppermute(home[:, :ROW_GROUPS], "tx", [(g, g - 1) for g in range(1, group_count)])
    in_vmem = pl.BlockSpec(memory_space=pltpu.VMEM)
    return pl.pallas_call(
        join_kernel,
        out_shape=jax.ShapeDtypeStruct((STRIDE, STRIDE * GROUP_COLS), jnp.float32),
        in_specs=[in_vmem, in_vmem], out_specs=in_vmem,
        compiler_params=pltpu.CompilerParams(vmem_limit_bytes=SMALL_VMEM),
        name="join",
    )(home, strip)


def solution(mesh):
    in_specs = (
        P("tx", "ty", None, None, None, None),
        P("tx", "ty", None, None),
        P("tx", "ty", None),
        P("tx", "ty"),
        P(),
        P(),
    )
    return jax.shard_map(
        shards, mesh=mesh, in_specs=in_specs, out_specs=P("ty", "tx"), check_vma=False
    )
```

```python
import functools
import math

import jax
import jax.numpy as jnp
import numpy as np
from jax import lax
from jax.experimental import pallas as pl
from jax.experimental.pallas import tpu as pltpu
from jax.sharding import PartitionSpec as P

SIDE = 384
STRIDE = 320
OVERLAP = SIDE - STRIDE
GROUP_COLS = 2
PHASES = 5
CELLS = 12
WIENER = 0.1
SHIFT_ROWS, SHIFT_COLS = 37, 101
CHUNK = SIDE // 16
SMALL_VMEM = 4 << 20
GROUP = 8
ROW_GROUPS = CHUNK // GROUP
TILE_GROUPS = 3 * ROW_GROUPS

NYQUIST = SIDE // 2
THIRD = SIDE // 3
HALF = SIDE // 2
BY_THREE = [np.arange(rest, HALF, 3) for rest in range(3)]


def cos_sin(rows, cols):
    angle = (np.outer(rows, cols) % SIDE) * (2.0 * math.pi / SIDE)
    return np.cos(angle), np.sin(angle)


def plus(cols):
    c, s = cos_sin(np.arange(THIRD), cols)
    return np.concatenate([c, s]), np.concatenate([-s, c])


def minus(cols):
    c, s = cos_sin(np.arange(THIRD), cols)
    return np.concatenate([c, -s]), np.concatenate([-s, -c])


def beside(blocks):
    return np.concatenate([b[0] for b in blocks] + [b[1] for b in blocks], axis=1)


def column_class(order, rest):
    return (rest - order * SHIFT_COLS) % 3


def first_tables():
    tables = []
    for order in (1, 2):
        move = order * SHIFT_COLS
        for rest in range(3):
            at = column_class(order, rest)
            if at == 0:
                blocks = [
                    plus(BY_THREE[0] + move), plus(np.array([NYQUIST + move])), minus(BY_THREE[0][1:] - move)
                ]
            elif at == 1:
                blocks = [plus(BY_THREE[1] + move), minus(BY_THREE[2] - move)]
            else:
                blocks = [minus(BY_THREE[1] - move), plus(BY_THREE[2] + move)]
            tables.append(beside(blocks))
    tables.append(beside([plus(BY_THREE[1]), minus(BY_THREE[2])]))
    blank = np.zeros((2 * THIRD, 63))
    tables.append(beside([plus(BY_THREE[0]), plus(np.array([NYQUIST])), (blank, blank)])[:THIRD])
    return np.concatenate(tables)


def row_tables():
    every = np.arange(HALF)
    tables = []
    for rows, cols in ((2 * every, every), (2 * every + 1, every)):
        c, s = cos_sin(rows, cols)
        tables.append(np.block([[c, s], [-s, c]]))
    return np.concatenate(tables)


def last_table():
    lines = np.concatenate([BY_THREE[1], BY_THREE[2], BY_THREE[0], [NYQUIST], BY_THREE[0][1:]])
    c, s = cos_sin(lines, np.arange(SIDE))
    return np.concatenate([c, s], axis=0)


def table(values):
    return jnp.asarray(values.astype(np.float32)).astype(jnp.bfloat16)


def dot(x, w):
    return jnp.dot(x, w, preferred_element_type=jnp.float32)


def halves(x):
    high = x.astype(jnp.bfloat16)
    return high, (x - high.astype(jnp.float32)).astype(jnp.bfloat16)


def negating(x_ref, flip, half_ref, back_ref):
    width = back_ref.shape[1]

    def over_rows(part):
        lanes = pl.ds(256 * part, 256)
        half_ref[:, lanes] = dot(flip, half_ref[:, lanes]).astype(jnp.bfloat16)

    def split():
        high, low = halves(x_ref[...])
        half_ref[:, 0:SIDE] = high
        half_ref[:, SIDE : 2 * SIDE] = low
        over_rows(0)

    def over_columns(low, high):
        here = flip[:, low:high]
        back_ref[:, low:high] = dot(half_ref[:, 0:SIDE], here) + dot(half_ref[:, SIDE : 2 * SIDE], here)

    steps = [split, functools.partial(over_rows, 1), functools.partial(over_rows, 2)]
    steps.append(functools.partial(over_columns, 0, 256))
    if width > 256:
        steps.append(functools.partial(over_columns, 256, width))
    return steps


def flip_matrix():
    rows = lax.broadcasted_iota(jnp.int32, (SIDE, SIDE), 0)
    cols = lax.broadcasted_iota(jnp.int32, (SIDE, SIDE), 1)
    total = rows + cols
    return ((total == 0) | (total == SIDE)).astype(jnp.float32).astype(jnp.bfloat16)


def class_matrix():
    rows = lax.broadcasted_iota(jnp.int32, (256, 256), 0)
    lane = lax.broadcasted_iota(jnp.int32, (256, 256), 1)
    wanted = jnp.where(lane < 64, 3 * lane + 1, jnp.where(lane < 128, 3 * lane - 190, 3 * lane - 384))
    wanted = jnp.where(lane == NYQUIST, NYQUIST, jnp.where(lane > NYQUIST, -1, wanted))
    return (rows == wanted).astype(jnp.float32).astype(jnp.bfloat16)


def filling(source_ref, numerator_ref, work_ref, gains_ref, first):
    def move(at):
        order = at - 2
        one = source_ref[...]
        if order:
            one = pltpu.roll(one, (-order * SHIFT_COLS) % SIDE, 1)[:, 0:256]
            one = pltpu.roll(one, (-order * SHIFT_ROWS) % SIDE, 0)
        work_ref[at] = one[:, 0:256]

    def scale(part):
        rows = pl.ds(128 * part, 128)
        power = WIENER + sum(work_ref[at, rows, :] * work_ref[at, rows, :] for at in range(5))
        weight = numerator_ref[rows, 0:256] / power
        for at in range(5):
            there = pl.ds(SIDE * at + 128 * part, 128)
            if first:
                gains_ref[there, :] = work_ref[at, rows, :] * weight
            else:
                gains_ref[there, :] += work_ref[at, rows, :] * weight

    return [functools.partial(move, at) for at in range(5)] + [functools.partial(scale, at) for at in range(3)]


def interleaved(few, many):
    done = 0
    for at, step in enumerate(few):
        step()
        until = (at + 1) * len(many) // len(few)
        for other in many[done:until]:
            other()
        done = until


def pack_gains(work_ref, gains_ref):
    lane = lax.broadcasted_iota(jnp.int32, (HALF, 128), 1)
    low = lane < 64
    nyquist = lane == 64
    for odd in range(2):
        rows = pl.ds(HALF * odd, HALF)

        def tiles(order):
            base = 2 * SIDE * (order + 2) + odd
            return tuple(work_ref[pl.ds(base + at, HALF, stride=2), :] for at in (0, SIDE))

        for order in (1, 2):
            base = 256 * (order - 1)
            up0, up1 = tiles(order)
            down0, down1 = tiles(-order)
            gains_ref[rows, base : base + 128] = jnp.where(low, up0, down0)
            gains_ref[rows, base + 128 : base + 256] = jnp.where(low, down0, up0)
            rest = jnp.where(low, up1, jnp.where(nyquist, up1, pltpu.roll(down1, 64, 1)))
            gains_ref[rows, 384 + 128 * order : 512 + 128 * order] = rest
        mid0, mid1 = tiles(0)
        gains_ref[rows, 768:896] = mid0
        edge = jnp.where(lane == 0, 0.5 * mid1, mid1)
        gains_ref[rows, 896:1024] = jnp.where(low, edge, jnp.where(nyquist, 0.5 * mid1, 0.0))


def tile_kernel(
    devices, group_count,
    names_ref, phases_ref,
    frames_hbm, masks_hbm, otf_hbm, apod_hbm, rows_hbm, cols_hbm, first_hbm, fwd_hbm, last_hbm,
    out_hbm,
    frames_ref, masks_ref, otf_ref, apod_ref, rows_ref, cols_ref, first_ref, fwd_ref, last_ref,
    work_ref, natural_ref, sorted_ref, gains_ref, half_ref, back_ref, back_apod_ref,
    left_a_ref, left_b_ref, y_ref, s_ref, t_ref, mid_ref, out_ref, tags_ref, sems,
):
    f32, bf16 = jnp.float32, jnp.bfloat16
    k1, k2 = math.cos(2 * math.pi / 5), math.cos(4 * math.pi / 5)
    n1, n2 = math.sin(2 * math.pi / 5), math.sin(4 * math.pi / 5)
    slots = frames_ref.shape[0]

    fixed = [
        (otf_hbm, otf_ref), (apod_hbm, apod_ref), (masks_hbm, masks_ref), (rows_hbm, rows_ref),
        (cols_hbm, cols_ref), (first_hbm, first_ref), (fwd_hbm, fwd_ref), (last_hbm, last_ref),
    ]
    early = 5
    left_refs = (left_a_ref, left_b_ref)

    def fixed_copy(at):
        return pltpu.make_async_copy(fixed[at][0], fixed[at][1], sems.at[at])

    def frame_copy(at):
        return pltpu.make_async_copy(frames_hbm.at[at], frames_ref.at[at], sems.at[len(fixed) + at])

    def out_copy(at):
        there = out_hbm.at[:, pl.ds(TILE_GROUPS * at, TILE_GROUPS)]
        return pltpu.make_async_copy(out_ref.at[at], there, sems.at[len(fixed) + slots + at])

    tags_copy = pltpu.make_async_copy(
        tags_ref, out_hbm.at[:, pl.ds(TILE_GROUPS * slots, 1)], sems.at[len(fixed) + 2 * slots]
    )

    def mixing(now):
        phase = jnp.full((GROUP, 128), phases_ref[0, now], f32)
        turns = [[fn(order * phase)[0:1, 0:1] for fn in (jnp.cos, jnp.sin)] for order in (1.0, 2.0)]
        cell_row = lax.broadcasted_iota(jnp.int32, (CELLS, SIDE), 0)
        cell_col = lax.broadcasted_iota(jnp.int32, (CELLS, SIDE), 1) // (SIDE // CELLS)
        spread = (cell_row == cell_col).astype(f32).astype(bf16)
        held = jnp.concatenate([masks_ref[now, row] for row in range(CELLS)], axis=0)
        flags = dot(held.astype(f32).astype(bf16), spread)

        def thirds(x):
            a, b, c = x[:, 0:128], x[:, 128:256], x[:, 256:384]
            both = b + c
            return a + both, a - 0.5 * both, (0.5 * math.sqrt(3.0)) * (b - c)

        def step(part):
            rows = pl.ds(16 * part, 16)
            flag = jnp.broadcast_to(flags[part // 2 : part // 2 + 1, :], (16, SIDE)).astype(bf16)
            f = [(frames_ref[now, p, rows, :] * flag).astype(f32) for p in range(PHASES)]
            a1, d1, a2, d2 = f[1] + f[4], f[1] - f[4], f[2] + f[3], f[2] - f[3]

            def put(at, value):
                left_refs[now % 2][rows, 128 * at : 128 * at + 128] = value.astype(bf16)

            total, even, odd = thirds((f[0] + a1 + a2) * (1.0 / PHASES))
            put(12, even)
            put(13, -odd)
            put(14, total)
            for at, (a, b) in enumerate((
                (f[0] + k1 * a1 + k2 * a2, n1 * d1 + n2 * d2),
                (f[0] + k2 * a1 + k1 * a2, n2 * d1 - n1 * d2),
            )):
                turn_c, turn_s = turns[at]
                row_c, row_s = rows_ref[rows, 2 + 2 * at : 3 + 2 * at], rows_ref[rows, 3 + 2 * at : 4 + 2 * at]
                c = turn_c * row_c - turn_s * row_s
                s = turn_s * row_c + turn_c * row_s
                total_r, even_r, odd_r = thirds(c * a - s * b)
                total_i, even_i, odd_i = thirds(-c * b - s * a)
                put(6 * at, total_r)
                put(6 * at + 1, total_i)
                put(6 * at + 2, even_r + odd_i)
                put(6 * at + 3, even_i - odd_r)
                put(6 * at + 4, even_r - odd_i)
                put(6 * at + 5, even_i + odd_r)

        return [functools.partial(step, part) for part in range(SIDE // 16)]

    def transform(slot, waiting):
        def mix_some(count):
            for step in waiting[:count]:
                step()
            del waiting[:count]

        def put_rows(r, col):
            for half in range(2):
                top = r[0:HALF, 128 * half : 128 * half + 128]
                bottom = r[HALF:SIDE, 128 * half : 128 * half + 128]
                base = HALF * half
                y_ref[base : base + HALF, col : col + 128] = (top + bottom).astype(bf16)
                y_ref[SIDE + base : SIDE + base + HALF, col : col + 128] = (top - bottom).astype(bf16)

        for at in range(2):
            columns = (512 + 128 * at, 256 * at, 256 * at + 128)
            for rest in range(3):
                k = 768 * at + 256 * rest
                r = dot(left_refs[slot % 2][:, k : k + 256], first_ref[k : k + 256, :])
                put_rows(r, columns[column_class(at + 1, rest)])
                mix_some(1)
        put_rows(dot(left_refs[slot % 2][:, 1536:1792], first_ref[1536:1792, :]), 768)
        mix_some(1)
        put_rows(dot(left_refs[slot % 2][:, 1792:1920], first_ref[1792:1920, :]), 896)
        mix_some(1)

        for odd in range(2):
            rows = pl.ds(SIDE * odd, SIDE)
            gain_rows = pl.ds(HALF * odd, HALF)
            for n in range(4):
                lanes = pl.ds(256 * n, 256)
                product = dot(fwd_ref[rows, :], y_ref[rows, lanes])
                g = gains_ref[gain_rows, lanes]
                for half in range(2):
                    d = product[HALF * half : HALF * half + HALF] * g
                    here = pl.ds(HALF * half, HALF)
                    if n == 0:
                        t_ref[here, 0:128] = d[:, 0:128] + d[:, 128:256]
                    elif n == 1:
                        t_ref[here, 0:128] += d[:, 0:128] + d[:, 128:256]
                    elif n == 2:
                        t_ref[here, 128:256] = d[:, 0:128] + d[:, 128:256]
                    else:
                        total = t_ref[here, :] + d
                        total = -total if half > odd else total
                        base = SIDE * odd + HALF * half
                        s_ref[base : base + HALF, :] = total.astype(bf16)
                mix_some(2)

        even_part = dot(fwd_ref[0:SIDE, :], s_ref[0:SIDE, :])
        odd_part = lax.dot_general(
            fwd_ref[SIDE : 2 * SIDE, :], s_ref[SIDE : 2 * SIDE, :], (((0,), (0,)), ((), ())),
            preferred_element_type=f32,
        )
        mix_some(len(waiting))
        for half in range(2):
            e, o = even_part[HALF * half : HALF * half + HALF], odd_part[HALF * half : HALF * half + HALF]
            o = -o if half else o
            lanes = pl.ds(256 * half, 256)
            mid_ref[0:HALF, lanes] = (e + o).astype(bf16)
            mid_ref[HALF:SIDE, lanes] = (e - o).astype(bf16)
        picture = dot(mid_ref[...], last_ref[...])
        name = names_ref[0, slot]
        row_last = name >= GROUP_COLS * (devices - 1)
        col_last = (lax.axis_index("tx") == group_count - 1) & (lax.rem(name, GROUP_COLS) == GROUP_COLS - 1)
        row_ramp = rows_ref[:, 0:1] * jnp.where(row_last, 1.0, rows_ref[:, 1:2])
        col_ramp = cols_ref[0:1, :] * jnp.where(col_last, 1.0, cols_ref[1:2, :])
        weighted = picture * row_ramp * col_ramp
        for part in range(SIDE // GROUP):
            chunk, i = part // ROW_GROUPS, part % ROW_GROUPS
            for tile in range(3):
                piece = weighted[GROUP * part : GROUP * part + GROUP, 128 * tile : 128 * tile + 128]
                out_ref[slot, chunk, ROW_GROUPS * tile + i] = piece.astype(bf16)
        out_copy(slot).start()

    for at in range(early):
        fixed_copy(at).start()
    frame_copy(0).start()
    line = lax.broadcasted_iota(jnp.int32, (GROUP, 128), 0)
    tags = jnp.full((GROUP, 128), -1.0, f32)
    for at in range(slots):
        tags = jnp.where(line == at, names_ref[0, at].astype(f32), tags)
    for chunk in range(devices):
        tags_ref[chunk, 0] = tags.astype(bf16)
    tags_copy.start()
    flip = flip_matrix()
    for at in range(early):
        fixed_copy(at).wait()
    for at in range(early, len(fixed)):
        fixed_copy(at).start()
    turning = negating(otf_ref, flip, half_ref, back_ref)
    interleaved(turning, filling(otf_ref, apod_ref, work_ref, natural_ref, True))
    frame_copy(0).wait()
    for at in range(1, slots):
        frame_copy(at).start()
    interleaved(negating(apod_ref, flip, half_ref, back_apod_ref), mixing(0))
    for step in filling(back_ref, back_apod_ref, work_ref, natural_ref, False):
        step()
    classes = class_matrix()
    for at in range(5):
        rows = pl.ds(SIDE * at, SIDE)
        high, low = halves(natural_ref[rows, :])
        sorted_gains = dot(high, classes) + dot(low, classes)
        for half in range(2):
            there = pl.ds(SIDE * (2 * at + half), SIDE)
            sorted_ref[there, :] = sorted_gains[:, 128 * half : 128 * half + 128]
    pack_gains(sorted_ref, gains_ref)
    for at in range(early, len(fixed)):
        fixed_copy(at).wait()

    for slot in range(slots):
        waiting = []
        if slot + 1 < slots:
            frame_copy(slot + 1).wait()
            waiting = mixing(slot + 1)
        transform(slot, waiting)
    tags_copy.wait()
    for at in range(slots):
        out_copy(at).wait()


def row_constants():
    places = np.arange(SIDE) + 0.5
    rising = np.minimum(places / OVERLAP, 1.0)
    falling = np.minimum((SIDE - places) / OVERLAP, 1.0)
    columns = [rising / (SIDE * SIDE), falling]
    for order in (1, 2):
        angle = (np.arange(SIDE) * order * SHIFT_ROWS % SIDE) * (2 * math.pi / SIDE)
        columns += [np.cos(angle) / PHASES, np.sin(angle) / PHASES]
    return np.stack(columns, axis=1), np.stack([rising, falling])


def tile_results(frames, masks, phases, names, otf, apod, devices, group_count):
    slots = frames.shape[0]
    f32, bf16 = jnp.float32, jnp.bfloat16
    rows, cols = (jnp.asarray(one, f32) for one in row_constants())
    tables = [table(one) for one in (first_tables(), row_tables(), last_table())]
    places = pl.BlockSpec(memory_space=pl.ANY)

    def like(array):
        return pltpu.VMEM(array.shape, array.dtype)

    given = [frames, masks, otf, apod, rows, cols] + tables
    return pl.pallas_call(
        functools.partial(tile_kernel, devices, group_count),
        out_shape=jax.ShapeDtypeStruct((devices, TILE_GROUPS * slots + 1, GROUP, 128), bf16),
        in_specs=[pl.BlockSpec(memory_space=pltpu.SMEM)] * 2 + [places] * len(given),
        out_specs=places,
        scratch_shapes=[like(one) for one in given] + [
            pltpu.VMEM((5, SIDE, 256), f32),
            pltpu.VMEM((5 * SIDE, 256), f32),
            pltpu.VMEM((10 * SIDE, 128), f32),
            pltpu.VMEM((SIDE, 1024), f32),
            pltpu.VMEM((SIDE, 2 * SIDE), bf16),
            pltpu.VMEM((SIDE, SIDE), f32),
            pltpu.VMEM((SIDE, 256), f32),
            pltpu.VMEM((SIDE, 1920), bf16),
            pltpu.VMEM((SIDE, 1920), bf16),
            pltpu.VMEM((2 * SIDE, 1024), bf16),
            pltpu.VMEM((2 * SIDE, 256), bf16),
            pltpu.VMEM((SIDE, 256), f32),
            pltpu.VMEM((SIDE, 512), bf16),
            pltpu.VMEM((slots, devices, TILE_GROUPS, GROUP, 128), bf16),
            pltpu.VMEM((devices, 1, GROUP, 128), bf16),
            pltpu.SemaphoreType.DMA((len(given) + 2 * slots,)),
        ],
        cost_estimate=pl.CostEstimate(flops=slots * 2_000_000_000, bytes_accessed=10_000_000, transcendentals=0),
        name="tiles",
    )(names, phases, *given)


def pick_kernel(slots, devices, in_ref, out_ref, where_ref, place_ref, sem):
    me = lax.axis_index("ty")
    per_device = TILE_GROUPS * slots + 1
    line = lax.broadcasted_iota(jnp.int32, (GROUP, 128), 0)
    lane = lax.broadcasted_iota(jnp.int32, (GROUP, 128), 1).astype(jnp.float32)
    place = jnp.zeros((GROUP, 128), jnp.int32)
    for source in range(devices):
        tags = in_ref[per_device * source + per_device - 1].astype(jnp.float32)
        place += jnp.where(tags == lane, per_device * source + TILE_GROUPS * line, 0)
    where_ref[...] = jnp.sum(place, axis=0, keepdims=True)
    copy = pltpu.make_async_copy(where_ref, place_ref, sem)
    copy.start()
    copy.wait()

    for i in range(ROW_GROUPS):
        ahead = (ROW_GROUPS * me + i < OVERLAP // GROUP).astype(jnp.int32)
        for target in range(devices):
            row = target + ahead
            for col in range(GROUP_COLS):
                source = place_ref[0, GROUP_COLS * row + col] + i
                for tile in range(3):
                    value = in_ref[source + ROW_GROUPS * tile]
                    if target == devices - 1:
                        value = jnp.where(row < devices, value, jnp.zeros_like(value))
                    out_ref[TILE_GROUPS * (GROUP_COLS * target + col) + ROW_GROUPS * tile + i] = value


def picked(spread, slots):
    devices = spread.shape[0]
    chosen = pl.pallas_call(
        functools.partial(pick_kernel, slots, devices),
        out_shape=jax.ShapeDtypeStruct((devices * GROUP_COLS * TILE_GROUPS, GROUP, 128), spread.dtype),
        in_specs=[pl.BlockSpec(memory_space=pltpu.VMEM)],
        out_specs=pl.BlockSpec(memory_space=pltpu.VMEM),
        scratch_shapes=[
            pltpu.VMEM((1, 128), jnp.int32), pltpu.SMEM((1, 128), jnp.int32), pltpu.SemaphoreType.DMA,
        ],
        compiler_params=pltpu.CompilerParams(vmem_limit_bytes=SMALL_VMEM),
        name="pick",
    )(spread.reshape(-1, GROUP, 128))
    return chosen.reshape(devices, -1, GROUP, 128)


def folded(in_ref, base):
    rows = []
    for part in range(SIDE // GROUP):
        value = in_ref[part // ROW_GROUPS, base + part % ROW_GROUPS]
        rows.append(value.astype(jnp.float32))
    count = OVERLAP // GROUP
    body = rows[count:]
    for at in range(count):
        body[len(body) - count + at] = body[len(body) - count + at] + rows[at]
    return jnp.concatenate(body, axis=0)


def join_kernel(in_ref, strip_ref, out_ref):
    low = lax.broadcasted_iota(jnp.int32, (STRIDE, 128), 1) < OVERLAP
    left = [pltpu.roll(folded(in_ref, ROW_GROUPS * tile), OVERLAP, 1) for tile in range(3)]
    right = [folded(in_ref, TILE_GROUPS + ROW_GROUPS * tile) for tile in range(3)]
    out_ref[:, 0:128] = jnp.where(low, left[0], left[1])
    out_ref[:, 128:256] = jnp.where(low, left[1], left[2])
    out_ref[:, 256:384] = right[0] + jnp.where(low, left[2], 0.0)
    out_ref[:, 384:512] = right[1]
    strip = pltpu.roll(folded(strip_ref, 0), OVERLAP, 1)
    out_ref[:, 512:640] = right[2] + jnp.where(low, 0.0, strip)


def shards(frames, masks, phases, slot_tile, otf, apod):
    devices = lax.axis_size("ty")
    group_count = lax.axis_size("tx")
    slots = frames.shape[1]
    results = tile_results(
        frames[0, :, 0], masks[0][:, :, None, :], phases[:, :, 0], slot_tile, otf, apod, devices, group_count
    )
    spread = lax.all_to_all(results, "ty", 0, 0, tiled=True)
    home = lax.all_to_all(picked(spread, slots), "ty", 0, 0, tiled=True)
    strip = lax.ppermute(home[:, :ROW_GROUPS], "tx", [(g, g - 1) for g in range(1, group_count)])
    in_vmem = pl.BlockSpec(memory_space=pltpu.VMEM)
    return pl.pallas_call(
        join_kernel,
        out_shape=jax.ShapeDtypeStruct((STRIDE, STRIDE * GROUP_COLS), jnp.float32),
        in_specs=[in_vmem, in_vmem], out_specs=in_vmem,
        compiler_params=pltpu.CompilerParams(vmem_limit_bytes=SMALL_VMEM),
        name="join",
    )(home, strip)


def solution(mesh):
    in_specs = (
        P("tx", "ty", None, None, None, None),
        P("tx", "ty", None, None),
        P("tx", "ty", None),
        P("tx", "ty"),
        P(),
        P(),
    )
    return jax.shard_map(
        shards, mesh=mesh, in_specs=in_specs, out_specs=P("ty", "tx"), check_vma=False
    )
```

```python
import functools
import math

import jax
import jax.numpy as jnp
import numpy as np
from jax import lax
from jax.experimental import pallas as pl
from jax.experimental.pallas import tpu as pltpu
from jax.sharding import PartitionSpec as P

SIDE = 384
STRIDE = 320
OVERLAP = SIDE - STRIDE
GROUP_COLS = 2
PHASES = 5
CELLS = 12
WIENER = 0.1
SHIFT_ROWS, SHIFT_COLS = 37, 101
CHUNK = SIDE // 16
SMALL_VMEM = 4 << 20
GROUP = 8
ROW_GROUPS = CHUNK // GROUP
TILE_GROUPS = 3 * ROW_GROUPS

NYQUIST = SIDE // 2
THIRD = SIDE // 3
HALF = SIDE // 2
BY_THREE = [np.arange(rest, HALF, 3) for rest in range(3)]


def cos_sin(rows, cols):
    angle = (np.outer(rows, cols) % SIDE) * (2.0 * math.pi / SIDE)
    return np.cos(angle), np.sin(angle)


def plus(cols):
    c, s = cos_sin(np.arange(THIRD), cols)
    return np.concatenate([c, s]), np.concatenate([-s, c])


def minus(cols):
    c, s = cos_sin(np.arange(THIRD), cols)
    return np.concatenate([c, -s]), np.concatenate([-s, -c])


def beside(blocks):
    return np.concatenate([b[0] for b in blocks] + [b[1] for b in blocks], axis=1)


def column_class(order, rest):
    return (rest - order * SHIFT_COLS) % 3


def first_tables():
    tables = []
    for order in (1, 2):
        move = order * SHIFT_COLS
        for rest in range(3):
            at = column_class(order, rest)
            if at == 0:
                blocks = [
                    plus(BY_THREE[0] + move), plus(np.array([NYQUIST + move])), minus(BY_THREE[0][1:] - move)
                ]
            elif at == 1:
                blocks = [plus(BY_THREE[1] + move), minus(BY_THREE[2] - move)]
            else:
                blocks = [minus(BY_THREE[1] - move), plus(BY_THREE[2] + move)]
            tables.append(beside(blocks))
    tables.append(beside([plus(BY_THREE[1]), minus(BY_THREE[2])]))
    blank = np.zeros((2 * THIRD, 63))
    tables.append(beside([plus(BY_THREE[0]), plus(np.array([NYQUIST])), (blank, blank)])[:THIRD])
    return np.concatenate(tables)


def row_tables():
    every = np.arange(HALF)
    tables = []
    for rows, cols in ((2 * every, every), (2 * every + 1, every)):
        c, s = cos_sin(rows, cols)
        tables.append(np.block([[c, s], [-s, c]]))
    return np.concatenate(tables)


def last_table():
    lines = np.concatenate([BY_THREE[1], BY_THREE[2], BY_THREE[0], [NYQUIST], BY_THREE[0][1:]])
    c, s = cos_sin(lines, np.arange(SIDE))
    return np.concatenate([c, s], axis=0)


def table(values):
    return jnp.asarray(values.astype(np.float32)).astype(jnp.bfloat16)


def dot(x, w):
    return jnp.dot(x, w, preferred_element_type=jnp.float32)


def halves(x):
    high = x.astype(jnp.bfloat16)
    return high, (x - high.astype(jnp.float32)).astype(jnp.bfloat16)


def negating(x_ref, flip, half_ref, back_ref):
    width = back_ref.shape[1]

    def over_rows(part):
        lanes = pl.ds(256 * part, 256)
        half_ref[:, lanes] = dot(flip, half_ref[:, lanes]).astype(jnp.bfloat16)

    def split():
        high, low = halves(x_ref[...])
        half_ref[:, 0:SIDE] = high
        half_ref[:, SIDE : 2 * SIDE] = low
        over_rows(0)

    def over_columns(low, high):
        here = flip[:, low:high]
        back_ref[:, low:high] = dot(half_ref[:, 0:SIDE], here) + dot(half_ref[:, SIDE : 2 * SIDE], here)

    steps = [split, functools.partial(over_rows, 1), functools.partial(over_rows, 2)]
    steps.append(functools.partial(over_columns, 0, 256))
    if width > 256:
        steps.append(functools.partial(over_columns, 256, width))
    return steps


def flip_matrix():
    rows = lax.broadcasted_iota(jnp.int32, (SIDE, SIDE), 0)
    cols = lax.broadcasted_iota(jnp.int32, (SIDE, SIDE), 1)
    total = rows + cols
    return ((total == 0) | (total == SIDE)).astype(jnp.float32).astype(jnp.bfloat16)


def class_matrix():
    rows = lax.broadcasted_iota(jnp.int32, (256, 256), 0)
    lane = lax.broadcasted_iota(jnp.int32, (256, 256), 1)
    wanted = jnp.where(lane < 64, 3 * lane + 1, jnp.where(lane < 128, 3 * lane - 190, 3 * lane - 384))
    wanted = jnp.where(lane == NYQUIST, NYQUIST, jnp.where(lane > NYQUIST, -1, wanted))
    return (rows == wanted).astype(jnp.float32).astype(jnp.bfloat16)


def filling(source_ref, numerator_ref, work_ref, gains_ref, first):
    def move(at):
        order = at - 2
        one = source_ref[...]
        if order:
            one = pltpu.roll(one, (-order * SHIFT_COLS) % SIDE, 1)[:, 0:256]
            one = pltpu.roll(one, (-order * SHIFT_ROWS) % SIDE, 0)
        work_ref[at] = one[:, 0:256]

    def scale(part):
        rows = pl.ds(128 * part, 128)
        power = WIENER + sum(work_ref[at, rows, :] * work_ref[at, rows, :] for at in range(5))
        weight = numerator_ref[rows, 0:256] / power
        for at in range(5):
            there = pl.ds(SIDE * at + 128 * part, 128)
            if first:
                gains_ref[there, :] = work_ref[at, rows, :] * weight
            else:
                gains_ref[there, :] += work_ref[at, rows, :] * weight

    return [functools.partial(move, at) for at in range(5)] + [functools.partial(scale, at) for at in range(3)]


def interleaved(few, many):
    done = 0
    for at, step in enumerate(few):
        step()
        until = (at + 1) * len(many) // len(few)
        for other in many[done:until]:
            other()
        done = until


def pack_gains(work_ref, gains_ref):
    lane = lax.broadcasted_iota(jnp.int32, (HALF, 128), 1)
    low = lane < 64
    nyquist = lane == 64
    for odd in range(2):
        rows = pl.ds(HALF * odd, HALF)

        def tiles(order):
            base = 2 * SIDE * (order + 2) + odd
            return tuple(work_ref[pl.ds(base + at, HALF, stride=2), :] for at in (0, SIDE))

        for order in (1, 2):
            base = 256 * (order - 1)
            up0, up1 = tiles(order)
            down0, down1 = tiles(-order)
            gains_ref[rows, base : base + 128] = jnp.where(low, up0, down0)
            gains_ref[rows, base + 128 : base + 256] = jnp.where(low, down0, up0)
            rest = jnp.where(low, up1, jnp.where(nyquist, up1, pltpu.roll(down1, 64, 1)))
            gains_ref[rows, 384 + 128 * order : 512 + 128 * order] = rest
        mid0, mid1 = tiles(0)
        gains_ref[rows, 768:896] = mid0
        edge = jnp.where(lane == 0, 0.5 * mid1, mid1)
        gains_ref[rows, 896:1024] = jnp.where(low, edge, jnp.where(nyquist, 0.5 * mid1, 0.0))


def tile_kernel(
    devices, group_count,
    names_ref, phases_ref,
    frames_hbm, masks_hbm, otf_hbm, apod_hbm, rows_hbm, cols_hbm, first_hbm, fwd_hbm, last_hbm,
    out_hbm,
    frames_ref, masks_ref, otf_ref, apod_ref, rows_ref, cols_ref, first_ref, fwd_ref, last_ref,
    work_ref, natural_ref, sorted_ref, gains_ref, half_ref, back_ref, back_apod_ref,
    left_a_ref, left_b_ref, y_ref, s_ref, t_ref, mid_ref, out_ref, tags_ref, sems,
):
    f32, bf16 = jnp.float32, jnp.bfloat16
    n1, n2 = math.sin(2 * math.pi / 5), math.sin(4 * math.pi / 5)
    slots = frames_ref.shape[0]

    fixed = [
        (otf_hbm, otf_ref), (apod_hbm, apod_ref), (masks_hbm, masks_ref), (rows_hbm, rows_ref),
        (cols_hbm, cols_ref), (first_hbm, first_ref), (fwd_hbm, fwd_ref), (last_hbm, last_ref),
    ]
    early = 5
    left_refs = (left_a_ref, left_b_ref)

    def fixed_copy(at):
        return pltpu.make_async_copy(fixed[at][0], fixed[at][1], sems.at[at])

    def frame_copy(at):
        return pltpu.make_async_copy(frames_hbm.at[at], frames_ref.at[at], sems.at[len(fixed) + at])

    def out_copy(at):
        there = out_hbm.at[:, pl.ds(TILE_GROUPS * at, TILE_GROUPS)]
        return pltpu.make_async_copy(out_ref.at[at], there, sems.at[len(fixed) + slots + at])

    tags_copy = pltpu.make_async_copy(
        tags_ref, out_hbm.at[:, pl.ds(TILE_GROUPS * slots, 1)], sems.at[len(fixed) + 2 * slots]
    )

    def mixing(now):
        phase = jnp.full((GROUP, 128), phases_ref[0, now], f32)
        turns = [[fn(order * phase)[0:1, 0:1] for fn in (jnp.cos, jnp.sin)] for order in (1.0, 2.0)]
        cell_row = lax.broadcasted_iota(jnp.int32, (CELLS, SIDE), 0)
        cell_col = lax.broadcasted_iota(jnp.int32, (CELLS, SIDE), 1) // (SIDE // CELLS)
        spread = (cell_row == cell_col).astype(f32).astype(bf16)
        held = jnp.concatenate([masks_ref[now, row] for row in range(CELLS)], axis=0)
        flags = dot(held.astype(f32).astype(bf16), spread)

        def thirds(x):
            a, b, c = x[:, 0:128], x[:, 128:256], x[:, 256:384]
            both = b + c
            return a + both, a - 0.5 * both, (0.5 * math.sqrt(3.0)) * (b - c)

        def step(part):
            rows = pl.ds(32 * part, 32)
            flag = jnp.broadcast_to(flags[part : part + 1, :], (32, SIDE)).astype(bf16)
            f = [(frames_ref[now, p, rows, :] * flag).astype(f32) for p in range(PHASES)]
            a1, d1, a2, d2 = f[1] + f[4], f[1] - f[4], f[2] + f[3], f[2] - f[3]

            def put(at, value):
                left_refs[now % 2][rows, 128 * at : 128 * at + 128] = value.astype(bf16)

            both = a1 + a2
            total, even, odd = thirds((f[0] + both) * (1.0 / PHASES))
            base, apart = f[0] - 0.25 * both, (0.25 * math.sqrt(5.0)) * (a1 - a2)
            put(12, even)
            put(13, -odd)
            put(14, total)
            for at, (a, b) in enumerate((
                (base + apart, n1 * d1 + n2 * d2),
                (base - apart, n2 * d1 - n1 * d2),
            )):
                turn_c, turn_s = turns[at]
                row_c, row_s = rows_ref[rows, 2 + 2 * at : 3 + 2 * at], rows_ref[rows, 3 + 2 * at : 4 + 2 * at]
                c = turn_c * row_c - turn_s * row_s
                s = turn_s * row_c + turn_c * row_s
                total_r, even_r, odd_r = thirds(c * a - s * b)
                total_i, even_i, odd_i = thirds(-c * b - s * a)
                put(6 * at, total_r)
                put(6 * at + 1, total_i)
                put(6 * at + 2, even_r + odd_i)
                put(6 * at + 3, even_i - odd_r)
                put(6 * at + 4, even_r - odd_i)
                put(6 * at + 5, even_i + odd_r)

        return [functools.partial(step, part) for part in range(CELLS)]

    def transform(slot, waiting):
        def mix_some(count):
            for step in waiting[:count]:
                step()
            del waiting[:count]

        def put_rows(r, col):
            for half in range(2):
                top = r[0:HALF, 128 * half : 128 * half + 128]
                bottom = r[HALF:SIDE, 128 * half : 128 * half + 128]
                base = HALF * half
                y_ref[base : base + HALF, col : col + 128] = (top + bottom).astype(bf16)
                y_ref[SIDE + base : SIDE + base + HALF, col : col + 128] = (top - bottom).astype(bf16)

        for at in range(2):
            columns = (512 + 128 * at, 256 * at, 256 * at + 128)
            for rest in range(3):
                k = 768 * at + 256 * rest
                r = dot(left_refs[slot % 2][:, k : k + 256], first_ref[k : k + 256, :])
                put_rows(r, columns[column_class(at + 1, rest)])
                mix_some(2)
        put_rows(dot(left_refs[slot % 2][:, 1536:1792], first_ref[1536:1792, :]), 768)
        mix_some(1)
        put_rows(dot(left_refs[slot % 2][:, 1792:1920], first_ref[1792:1920, :]), 896)
        mix_some(1)

        for odd in range(2):
            rows = pl.ds(SIDE * odd, SIDE)
            gain_rows = pl.ds(HALF * odd, HALF)
            for n in range(4):
                lanes = pl.ds(256 * n, 256)
                product = dot(fwd_ref[rows, :], y_ref[rows, lanes])
                g = gains_ref[gain_rows, lanes]
                for half in range(2):
                    d = product[HALF * half : HALF * half + HALF] * g
                    here = pl.ds(HALF * half, HALF)
                    if n == 0:
                        t_ref[here, 0:128] = d[:, 0:128] + d[:, 128:256]
                    elif n == 1:
                        t_ref[here, 0:128] += d[:, 0:128] + d[:, 128:256]
                    elif n == 2:
                        t_ref[here, 128:256] = d[:, 0:128] + d[:, 128:256]
                    else:
                        total = t_ref[here, :] + d
                        total = -total if half > odd else total
                        base = SIDE * odd + HALF * half
                        s_ref[base : base + HALF, :] = total.astype(bf16)
                mix_some(1 if n % 2 else 0)

        even_part = dot(fwd_ref[0:SIDE, :], s_ref[0:SIDE, :])
        odd_part = lax.dot_general(
            fwd_ref[SIDE : 2 * SIDE, :], s_ref[SIDE : 2 * SIDE, :], (((0,), (0,)), ((), ())),
            preferred_element_type=f32,
        )
        mix_some(len(waiting))
        for half in range(2):
            e, o = even_part[HALF * half : HALF * half + HALF], odd_part[HALF * half : HALF * half + HALF]
            o = -o if half else o
            lanes = pl.ds(256 * half, 256)
            mid_ref[0:HALF, lanes] = (e + o).astype(bf16)
            mid_ref[HALF:SIDE, lanes] = (e - o).astype(bf16)
        picture = dot(mid_ref[...], last_ref[...])
        name = names_ref[0, slot]
        row_last = name >= GROUP_COLS * (devices - 1)
        col_last = (lax.axis_index("tx") == group_count - 1) & (lax.rem(name, GROUP_COLS) == GROUP_COLS - 1)
        row_ramp = rows_ref[:, 0:1] * jnp.where(row_last, 1.0, rows_ref[:, 1:2])
        col_ramp = cols_ref[0:1, :] * jnp.where(col_last, 1.0, cols_ref[1:2, :])
        weighted = picture * row_ramp * col_ramp
        for part in range(SIDE // GROUP):
            chunk, i = part // ROW_GROUPS, part % ROW_GROUPS
            for tile in range(3):
                piece = weighted[GROUP * part : GROUP * part + GROUP, 128 * tile : 128 * tile + 128]
                out_ref[slot, chunk, ROW_GROUPS * tile + i] = piece.astype(bf16)
        out_copy(slot).start()

    for at in range(early):
        fixed_copy(at).start()
    frame_copy(0).start()
    line = lax.broadcasted_iota(jnp.int32, (GROUP, 128), 0)
    tags = jnp.full((GROUP, 128), -1.0, f32)
    for at in range(slots):
        tags = jnp.where(line == at, names_ref[0, at].astype(f32), tags)
    for chunk in range(devices):
        tags_ref[chunk, 0] = tags.astype(bf16)
    tags_copy.start()
    flip = flip_matrix()
    for at in range(early):
        fixed_copy(at).wait()
    for at in range(early, len(fixed)):
        fixed_copy(at).start()
    turning = negating(otf_ref, flip, half_ref, back_ref)
    interleaved(turning, filling(otf_ref, apod_ref, work_ref, natural_ref, True))
    frame_copy(0).wait()
    for at in range(1, slots):
        frame_copy(at).start()
    interleaved(negating(apod_ref, flip, half_ref, back_apod_ref), mixing(0))
    for step in filling(back_ref, back_apod_ref, work_ref, natural_ref, False):
        step()
    classes = class_matrix()
    for at in range(5):
        rows = pl.ds(SIDE * at, SIDE)
        high, low = halves(natural_ref[rows, :])
        sorted_gains = dot(high, classes) + dot(low, classes)
        for half in range(2):
            there = pl.ds(SIDE * (2 * at + half), SIDE)
            sorted_ref[there, :] = sorted_gains[:, 128 * half : 128 * half + 128]
    pack_gains(sorted_ref, gains_ref)
    for at in range(early, len(fixed)):
        fixed_copy(at).wait()

    for slot in range(slots):
        waiting = []
        if slot + 1 < slots:
            frame_copy(slot + 1).wait()
            waiting = mixing(slot + 1)
        transform(slot, waiting)
    tags_copy.wait()
    for at in range(slots):
        out_copy(at).wait()


def row_constants():
    places = np.arange(SIDE) + 0.5
    rising = np.minimum(places / OVERLAP, 1.0)
    falling = np.minimum((SIDE - places) / OVERLAP, 1.0)
    columns = [rising / (SIDE * SIDE), falling]
    for order in (1, 2):
        angle = (np.arange(SIDE) * order * SHIFT_ROWS % SIDE) * (2 * math.pi / SIDE)
        columns += [np.cos(angle) / PHASES, np.sin(angle) / PHASES]
    return np.stack(columns, axis=1), np.stack([rising, falling])


def tile_results(frames, masks, phases, names, otf, apod, devices, group_count):
    slots = frames.shape[0]
    f32, bf16 = jnp.float32, jnp.bfloat16
    rows, cols = (jnp.asarray(one, f32) for one in row_constants())
    tables = [table(one) for one in (first_tables(), row_tables(), last_table())]
    places = pl.BlockSpec(memory_space=pl.ANY)

    def like(array):
        return pltpu.VMEM(array.shape, array.dtype)

    given = [frames, masks, otf, apod, rows, cols] + tables
    return pl.pallas_call(
        functools.partial(tile_kernel, devices, group_count),
        out_shape=jax.ShapeDtypeStruct((devices, TILE_GROUPS * slots + 1, GROUP, 128), bf16),
        in_specs=[pl.BlockSpec(memory_space=pltpu.SMEM)] * 2 + [places] * len(given),
        out_specs=places,
        scratch_shapes=[like(one) for one in given] + [
            pltpu.VMEM((5, SIDE, 256), f32),
            pltpu.VMEM((5 * SIDE, 256), f32),
            pltpu.VMEM((10 * SIDE, 128), f32),
            pltpu.VMEM((SIDE, 1024), f32),
            pltpu.VMEM((SIDE, 2 * SIDE), bf16),
            pltpu.VMEM((SIDE, SIDE), f32),
            pltpu.VMEM((SIDE, 256), f32),
            pltpu.VMEM((SIDE, 1920), bf16),
            pltpu.VMEM((SIDE, 1920), bf16),
            pltpu.VMEM((2 * SIDE, 1024), bf16),
            pltpu.VMEM((2 * SIDE, 256), bf16),
            pltpu.VMEM((SIDE, 256), f32),
            pltpu.VMEM((SIDE, 512), bf16),
            pltpu.VMEM((slots, devices, TILE_GROUPS, GROUP, 128), bf16),
            pltpu.VMEM((devices, 1, GROUP, 128), bf16),
            pltpu.SemaphoreType.DMA((len(given) + 2 * slots,)),
        ],
        cost_estimate=pl.CostEstimate(flops=slots * 2_000_000_000, bytes_accessed=10_000_000, transcendentals=0),
        name="tiles",
    )(names, phases, *given)


def pick_kernel(slots, devices, in_ref, out_ref, where_ref, place_ref, sem):
    me = lax.axis_index("ty")
    per_device = TILE_GROUPS * slots + 1
    line = lax.broadcasted_iota(jnp.int32, (GROUP, 128), 0)
    lane = lax.broadcasted_iota(jnp.int32, (GROUP, 128), 1).astype(jnp.float32)
    place = jnp.zeros((GROUP, 128), jnp.int32)
    for source in range(devices):
        tags = in_ref[per_device * source + per_device - 1].astype(jnp.float32)
        place += jnp.where(tags == lane, per_device * source + TILE_GROUPS * line, 0)
    where_ref[...] = jnp.sum(place, axis=0, keepdims=True)
    copy = pltpu.make_async_copy(where_ref, place_ref, sem)
    copy.start()
    copy.wait()

    for i in range(ROW_GROUPS):
        ahead = (ROW_GROUPS * me + i < OVERLAP // GROUP).astype(jnp.int32)
        for target in range(devices):
            row = target + ahead
            for col in range(GROUP_COLS):
                source = place_ref[0, GROUP_COLS * row + col] + i
                for tile in range(3):
                    value = in_ref[source + ROW_GROUPS * tile]
                    if target == devices - 1:
                        value = jnp.where(row < devices, value, jnp.zeros_like(value))
                    out_ref[TILE_GROUPS * (GROUP_COLS * target + col) + ROW_GROUPS * tile + i] = value


def picked(spread, slots):
    devices = spread.shape[0]
    chosen = pl.pallas_call(
        functools.partial(pick_kernel, slots, devices),
        out_shape=jax.ShapeDtypeStruct((devices * GROUP_COLS * TILE_GROUPS, GROUP, 128), spread.dtype),
        in_specs=[pl.BlockSpec(memory_space=pltpu.VMEM)],
        out_specs=pl.BlockSpec(memory_space=pltpu.VMEM),
        scratch_shapes=[
            pltpu.VMEM((1, 128), jnp.int32), pltpu.SMEM((1, 128), jnp.int32), pltpu.SemaphoreType.DMA,
        ],
        compiler_params=pltpu.CompilerParams(vmem_limit_bytes=SMALL_VMEM),
        name="pick",
    )(spread.reshape(-1, GROUP, 128))
    return chosen.reshape(devices, -1, GROUP, 128)


def folded(in_ref, base):
    rows = []
    for part in range(SIDE // GROUP):
        value = in_ref[part // ROW_GROUPS, base + part % ROW_GROUPS]
        rows.append(value.astype(jnp.float32))
    count = OVERLAP // GROUP
    body = rows[count:]
    for at in range(count):
        body[len(body) - count + at] = body[len(body) - count + at] + rows[at]
    return jnp.concatenate(body, axis=0)


def join_kernel(in_ref, strip_ref, out_ref):
    low = lax.broadcasted_iota(jnp.int32, (STRIDE, 128), 1) < OVERLAP
    left = [pltpu.roll(folded(in_ref, ROW_GROUPS * tile), OVERLAP, 1) for tile in range(3)]
    right = [folded(in_ref, TILE_GROUPS + ROW_GROUPS * tile) for tile in range(3)]
    out_ref[:, 0:128] = jnp.where(low, left[0], left[1])
    out_ref[:, 128:256] = jnp.where(low, left[1], left[2])
    out_ref[:, 256:384] = right[0] + jnp.where(low, left[2], 0.0)
    out_ref[:, 384:512] = right[1]
    strip = pltpu.roll(folded(strip_ref, 0), OVERLAP, 1)
    out_ref[:, 512:640] = right[2] + jnp.where(low, 0.0, strip)


def shards(frames, masks, phases, slot_tile, otf, apod):
    devices = lax.axis_size("ty")
    group_count = lax.axis_size("tx")
    slots = frames.shape[1]
    results = tile_results(
        frames[0, :, 0], masks[0][:, :, None, :], phases[:, :, 0], slot_tile, otf, apod, devices, group_count
    )
    spread = lax.all_to_all(results, "ty", 0, 0, tiled=True)
    home = lax.all_to_all(picked(spread, slots), "ty", 0, 0, tiled=True)
    strip = lax.ppermute(home[:, :ROW_GROUPS], "tx", [(g, g - 1) for g in range(1, group_count)])
    in_vmem = pl.BlockSpec(memory_space=pltpu.VMEM)
    return pl.pallas_call(
        join_kernel,
        out_shape=jax.ShapeDtypeStruct((STRIDE, STRIDE * GROUP_COLS), jnp.float32),
        in_specs=[in_vmem, in_vmem], out_specs=in_vmem,
        compiler_params=pltpu.CompilerParams(vmem_limit_bytes=SMALL_VMEM),
        name="join",
    )(home, strip)


def solution(mesh):
    in_specs = (
        P("tx", "ty", None, None, None, None),
        P("tx", "ty", None, None),
        P("tx", "ty", None),
        P("tx", "ty"),
        P(),
        P(),
    )
    return jax.shard_map(
        shards, mesh=mesh, in_specs=in_specs, out_specs=P("ty", "tx"), check_vma=False
    )
```

```python
import functools
import math

import jax
import jax.numpy as jnp
import numpy as np
from jax import lax
from jax.experimental import pallas as pl
from jax.experimental.pallas import tpu as pltpu
from jax.sharding import PartitionSpec as P

SIDE = 384
STRIDE = 320
OVERLAP = SIDE - STRIDE
GROUP_COLS = 2
PHASES = 5
CELLS = 12
WIENER = 0.1
SHIFT_ROWS, SHIFT_COLS = 37, 101
CHUNK = SIDE // 16
SMALL_VMEM = 4 << 20
GROUP = 8
ROW_GROUPS = CHUNK // GROUP
TILE_GROUPS = 3 * ROW_GROUPS

NYQUIST = SIDE // 2
THIRD = SIDE // 3
HALF = SIDE // 2
BY_THREE = [np.arange(rest, HALF, 3) for rest in range(3)]


def cos_sin(rows, cols):
    angle = (np.outer(rows, cols) % SIDE) * (2.0 * math.pi / SIDE)
    return np.cos(angle), np.sin(angle)


def plus(cols):
    c, s = cos_sin(np.arange(THIRD), cols)
    return np.concatenate([c, s]), np.concatenate([-s, c])


def minus(cols):
    c, s = cos_sin(np.arange(THIRD), cols)
    return np.concatenate([c, -s]), np.concatenate([-s, -c])


def beside(blocks):
    return np.concatenate([b[0] for b in blocks] + [b[1] for b in blocks], axis=1)


def column_class(order, rest):
    return (rest - order * SHIFT_COLS) % 3


def first_tables():
    tables = []
    for order in (1, 2):
        move = order * SHIFT_COLS
        for rest in range(3):
            at = column_class(order, rest)
            if at == 0:
                blocks = [
                    plus(BY_THREE[0] + move), plus(np.array([NYQUIST + move])), minus(BY_THREE[0][1:] - move)
                ]
            elif at == 1:
                blocks = [plus(BY_THREE[1] + move), minus(BY_THREE[2] - move)]
            else:
                blocks = [minus(BY_THREE[1] - move), plus(BY_THREE[2] + move)]
            tables.append(beside(blocks))
    tables.append(beside([plus(BY_THREE[1]), minus(BY_THREE[2])]))
    blank = np.zeros((2 * THIRD, 63))
    tables.append(beside([plus(BY_THREE[0]), plus(np.array([NYQUIST])), (blank, blank)])[:THIRD])
    return np.concatenate(tables)


def row_tables():
    every = np.arange(HALF)
    tables = []
    for rows, cols in ((2 * every, every), (2 * every + 1, every)):
        c, s = cos_sin(rows, cols)
        tables.append(np.block([[c, s], [-s, c]]))
    return np.concatenate(tables)


def last_table():
    lines = np.concatenate([BY_THREE[1], BY_THREE[2], BY_THREE[0], [NYQUIST], BY_THREE[0][1:]])
    c, s = cos_sin(lines, np.arange(SIDE))
    return np.concatenate([c, s], axis=0)


def table(values):
    return jnp.asarray(values.astype(np.float32)).astype(jnp.bfloat16)


def dot(x, w):
    return jnp.dot(x, w, preferred_element_type=jnp.float32)


def halves(x):
    high = x.astype(jnp.bfloat16)
    return high, (x - high.astype(jnp.float32)).astype(jnp.bfloat16)


def negating(x_ref, flip, half_ref, back_ref):
    width = back_ref.shape[1]

    def over_rows(part):
        lanes = pl.ds(256 * part, 256)
        half_ref[:, lanes] = dot(flip, half_ref[:, lanes]).astype(jnp.bfloat16)

    def split():
        high, low = halves(x_ref[...])
        half_ref[:, 0:SIDE] = high
        half_ref[:, SIDE : 2 * SIDE] = low
        over_rows(0)

    def over_columns(low, high):
        here = flip[:, low:high]
        back_ref[:, low:high] = dot(half_ref[:, 0:SIDE], here) + dot(half_ref[:, SIDE : 2 * SIDE], here)

    steps = [split, functools.partial(over_rows, 1), functools.partial(over_rows, 2)]
    steps.append(functools.partial(over_columns, 0, 256))
    if width > 256:
        steps.append(functools.partial(over_columns, 256, width))
    return steps


def flip_matrix():
    rows = lax.broadcasted_iota(jnp.int32, (SIDE, SIDE), 0)
    cols = lax.broadcasted_iota(jnp.int32, (SIDE, SIDE), 1)
    total = rows + cols
    return ((total == 0) | (total == SIDE)).astype(jnp.float32).astype(jnp.bfloat16)


def class_matrix():
    rows = lax.broadcasted_iota(jnp.int32, (256, 256), 0)
    lane = lax.broadcasted_iota(jnp.int32, (256, 256), 1)
    wanted = jnp.where(lane < 64, 3 * lane + 1, jnp.where(lane < 128, 3 * lane - 190, 3 * lane - 384))
    wanted = jnp.where(lane == NYQUIST, NYQUIST, jnp.where(lane > NYQUIST, -1, wanted))
    return (rows == wanted).astype(jnp.float32).astype(jnp.bfloat16)


def filling(source_ref, numerator_ref, work_ref, gains_ref, first):
    def move(at):
        order = at - 2
        one = source_ref[...]
        if order:
            one = pltpu.roll(one, (-order * SHIFT_COLS) % SIDE, 1)[:, 0:256]
            one = pltpu.roll(one, (-order * SHIFT_ROWS) % SIDE, 0)
        work_ref[at] = one[:, 0:256]

    def scale(part):
        rows = pl.ds(128 * part, 128)
        power = WIENER + sum(work_ref[at, rows, :] * work_ref[at, rows, :] for at in range(5))
        weight = numerator_ref[rows, 0:256] / power
        for at in range(5):
            there = pl.ds(SIDE * at + 128 * part, 128)
            if first:
                gains_ref[there, :] = work_ref[at, rows, :] * weight
            else:
                gains_ref[there, :] += work_ref[at, rows, :] * weight

    return [functools.partial(move, at) for at in range(5)] + [functools.partial(scale, at) for at in range(3)]


def interleaved(few, many):
    done = 0
    for at, step in enumerate(few):
        step()
        until = (at + 1) * len(many) // len(few)
        for other in many[done:until]:
            other()
        done = until


def pack_gains(work_ref, gains_ref):
    lane = lax.broadcasted_iota(jnp.int32, (HALF, 128), 1)
    low = lane < 64
    nyquist = lane == 64
    for odd in range(2):
        rows = pl.ds(HALF * odd, HALF)

        def tiles(order):
            base = 2 * SIDE * (order + 2) + odd
            return tuple(work_ref[pl.ds(base + at, HALF, stride=2), :] for at in (0, SIDE))

        for order in (1, 2):
            base = 256 * (order - 1)
            up0, up1 = tiles(order)
            down0, down1 = tiles(-order)
            gains_ref[rows, base : base + 128] = jnp.where(low, up0, down0)
            gains_ref[rows, base + 128 : base + 256] = jnp.where(low, down0, up0)
            rest = jnp.where(low, up1, jnp.where(nyquist, up1, pltpu.roll(down1, 64, 1)))
            gains_ref[rows, 384 + 128 * order : 512 + 128 * order] = rest
        mid0, mid1 = tiles(0)
        gains_ref[rows, 768:896] = mid0
        edge = jnp.where(lane == 0, 0.5 * mid1, mid1)
        gains_ref[rows, 896:1024] = jnp.where(low, edge, jnp.where(nyquist, 0.5 * mid1, 0.0))


def tile_kernel(
    devices, group_count,
    names_ref, phases_ref,
    frames_hbm, masks_hbm, otf_hbm, apod_hbm, rows_hbm, cols_hbm, first_hbm, fwd_hbm, last_hbm,
    out_hbm,
    frames_ref, masks_ref, otf_ref, apod_ref, rows_ref, cols_ref, first_ref, fwd_ref, last_ref,
    work_ref, natural_ref, sorted_ref, gains_ref, half_ref, back_ref, back_apod_ref,
    left_a_ref, left_b_ref, y_ref, s_ref, t_ref, mid_ref, out_ref, tags_ref, sems,
):
    f32, bf16 = jnp.float32, jnp.bfloat16
    n1, n2 = math.sin(2 * math.pi / 5), math.sin(4 * math.pi / 5)
    slots = frames_ref.shape[0]

    fixed = [
        (otf_hbm, otf_ref), (apod_hbm, apod_ref), (masks_hbm, masks_ref), (rows_hbm, rows_ref),
        (cols_hbm, cols_ref), (first_hbm, first_ref), (fwd_hbm, fwd_ref), (last_hbm, last_ref),
    ]
    early = 5
    left_refs = (left_a_ref, left_b_ref)

    def fixed_copy(at):
        return pltpu.make_async_copy(fixed[at][0], fixed[at][1], sems.at[at])

    def frame_copy(at):
        return pltpu.make_async_copy(frames_hbm.at[at], frames_ref.at[at], sems.at[len(fixed) + at])

    def out_copy(at):
        there = out_hbm.at[:, pl.ds(TILE_GROUPS * at, TILE_GROUPS)]
        return pltpu.make_async_copy(out_ref.at[at], there, sems.at[len(fixed) + slots + at])

    tags_copy = pltpu.make_async_copy(
        tags_ref, out_hbm.at[:, pl.ds(TILE_GROUPS * slots, 1)], sems.at[len(fixed) + 2 * slots]
    )

    def mixing(now):
        phase = jnp.full((GROUP, 128), phases_ref[0, now], f32)
        turns = [[fn(order * phase)[0:1, 0:1] for fn in (jnp.cos, jnp.sin)] for order in (1.0, 2.0)]
        cell_row = lax.broadcasted_iota(jnp.int32, (CELLS, SIDE), 0)
        cell_col = lax.broadcasted_iota(jnp.int32, (CELLS, SIDE), 1) // (SIDE // CELLS)
        spread = (cell_row == cell_col).astype(f32).astype(bf16)
        held = jnp.concatenate([masks_ref[now, row] for row in range(CELLS)], axis=0)
        flags = dot(held.astype(f32).astype(bf16), spread)

        def thirds(x):
            a, b, c = x[:, 0:128], x[:, 128:256], x[:, 256:384]
            both = b + c
            return a + both, a - 0.5 * both, (0.5 * math.sqrt(3.0)) * (b - c)

        def step(part):
            rows = pl.ds(32 * part, 32)
            flag = jnp.broadcast_to(flags[part : part + 1, :], (32, SIDE)).astype(bf16)
            f = [(frames_ref[now, p, rows, :] * flag).astype(f32) for p in range(PHASES)]
            a1, d1, a2, d2 = f[1] + f[4], f[1] - f[4], f[2] + f[3], f[2] - f[3]

            def put(at, value):
                left_refs[now % 2][rows, 128 * at : 128 * at + 128] = value.astype(bf16)

            both = a1 + a2
            total, even, odd = thirds((f[0] + both) * (1.0 / PHASES))
            base, apart = f[0] - 0.25 * both, (0.25 * math.sqrt(5.0)) * (a1 - a2)
            put(12, even)
            put(13, -odd)
            put(14, total)
            for at, (a, b) in enumerate((
                (base + apart, n1 * d1 + n2 * d2),
                (base - apart, n2 * d1 - n1 * d2),
            )):
                turn_c, turn_s = turns[at]
                row_c, row_s = rows_ref[rows, 2 + 2 * at : 3 + 2 * at], rows_ref[rows, 3 + 2 * at : 4 + 2 * at]
                c = turn_c * row_c - turn_s * row_s
                s = turn_s * row_c + turn_c * row_s
                total_r, even_r, odd_r = thirds(c * a - s * b)
                total_i, even_i, odd_i = thirds(-c * b - s * a)
                put(6 * at, total_r)
                put(6 * at + 1, total_i)
                put(6 * at + 2, even_r + odd_i)
                put(6 * at + 3, even_i - odd_r)
                put(6 * at + 4, even_r - odd_i)
                put(6 * at + 5, even_i + odd_r)

        return [functools.partial(step, part) for part in range(CELLS)]

    def transform(slot, waiting):
        def mix_some(count):
            for step in waiting[:count]:
                step()
            del waiting[:count]

        def put_rows(r, col):
            for half in range(2):
                top = r[0:HALF, 128 * half : 128 * half + 128]
                bottom = r[HALF:SIDE, 128 * half : 128 * half + 128]
                base = HALF * half
                y_ref[base : base + HALF, col : col + 128] = (top + bottom).astype(bf16)
                y_ref[SIDE + base : SIDE + base + HALF, col : col + 128] = (top - bottom).astype(bf16)

        for at in range(2):
            columns = (512 + 128 * at, 256 * at, 256 * at + 128)
            for rest in range(3):
                k = 768 * at + 256 * rest
                r = dot(left_refs[slot % 2][:, k : k + 256], first_ref[k : k + 256, :])
                put_rows(r, columns[column_class(at + 1, rest)])
                mix_some(2)
        put_rows(dot(left_refs[slot % 2][:, 1536:1792], first_ref[1536:1792, :]), 768)
        mix_some(1)
        put_rows(dot(left_refs[slot % 2][:, 1792:1920], first_ref[1792:1920, :]), 896)
        mix_some(1)

        for odd in range(2):
            rows = pl.ds(SIDE * odd, SIDE)
            gain_rows = pl.ds(HALF * odd, HALF)
            for n in range(4):
                lanes = pl.ds(256 * n, 256)
                product = dot(fwd_ref[rows, :], y_ref[rows, lanes])
                g = gains_ref[gain_rows, lanes]
                for half in range(2):
                    d = product[HALF * half : HALF * half + HALF] * g
                    here = pl.ds(HALF * half, HALF)
                    if n == 0:
                        t_ref[here, 0:128] = d[:, 0:128] + d[:, 128:256]
                    elif n == 1:
                        t_ref[here, 0:128] += d[:, 0:128] + d[:, 128:256]
                    elif n == 2:
                        t_ref[here, 128:256] = d[:, 0:128] + d[:, 128:256]
                    else:
                        total = t_ref[here, :] + d
                        total = -total if half > odd else total
                        base = SIDE * odd + HALF * half
                        s_ref[base : base + HALF, :] = total.astype(bf16)
                mix_some(1 if n % 2 else 0)

        even_part = dot(fwd_ref[0:SIDE, :], s_ref[0:SIDE, :])
        odd_part = lax.dot_general(
            fwd_ref[SIDE : 2 * SIDE, :], s_ref[SIDE : 2 * SIDE, :], (((0,), (0,)), ((), ())),
            preferred_element_type=f32,
        )
        mix_some(len(waiting))
        for half in range(2):
            e, o = even_part[HALF * half : HALF * half + HALF], odd_part[HALF * half : HALF * half + HALF]
            o = -o if half else o
            lanes = pl.ds(256 * half, 256)
            mid_ref[0:HALF, lanes] = (e + o).astype(bf16)
            mid_ref[HALF:SIDE, lanes] = (e - o).astype(bf16)
        picture = dot(mid_ref[...], last_ref[...])
        name = names_ref[0, slot]
        row_last = name >= GROUP_COLS * (devices - 1)
        col_last = (lax.axis_index("tx") == group_count - 1) & (lax.rem(name, GROUP_COLS) == GROUP_COLS - 1)
        row_ramp = rows_ref[:, 0:1] * jnp.where(row_last, 1.0, rows_ref[:, 1:2])
        col_ramp = cols_ref[0:1, :] * jnp.where(col_last, 1.0, cols_ref[1:2, :])
        weighted = picture * row_ramp * col_ramp
        for part in range(SIDE // GROUP):
            chunk, i = part // ROW_GROUPS, part % ROW_GROUPS
            for tile in range(3):
                piece = weighted[GROUP * part : GROUP * part + GROUP, 128 * tile : 128 * tile + 128]
                out_ref[slot, chunk, ROW_GROUPS * tile + i] = piece.astype(bf16)
        out_copy(slot).start()

    for at in range(early):
        fixed_copy(at).start()
    frame_copy(0).start()
    line = lax.broadcasted_iota(jnp.int32, (GROUP, 128), 0)
    tags = jnp.full((GROUP, 128), -1.0, f32)
    for at in range(slots):
        tags = jnp.where(line == at, names_ref[0, at].astype(f32), tags)
    for chunk in range(devices):
        tags_ref[chunk, 0] = tags.astype(bf16)
    tags_copy.start()
    flip = flip_matrix()
    for at in range(early):
        fixed_copy(at).wait()
    for at in range(early, len(fixed)):
        fixed_copy(at).start()
    turning = negating(otf_ref, flip, half_ref, back_ref)
    interleaved(turning, filling(otf_ref, apod_ref, work_ref, natural_ref, True))
    frame_copy(0).wait()
    for at in range(1, slots):
        frame_copy(at).start()
    interleaved(negating(apod_ref, flip, half_ref, back_apod_ref), mixing(0))
    for step in filling(back_ref, back_apod_ref, work_ref, natural_ref, False):
        step()
    classes = class_matrix()
    for at in range(5):
        rows = pl.ds(SIDE * at, SIDE)
        high, low = halves(natural_ref[rows, :])
        sorted_gains = dot(high, classes) + dot(low, classes)
        for half in range(2):
            there = pl.ds(SIDE * (2 * at + half), SIDE)
            sorted_ref[there, :] = sorted_gains[:, 128 * half : 128 * half + 128]
    pack_gains(sorted_ref, gains_ref)
    for at in range(early, len(fixed)):
        fixed_copy(at).wait()

    for slot in range(slots):
        waiting = []
        if slot + 1 < slots:
            frame_copy(slot + 1).wait()
            waiting = mixing(slot + 1)
        transform(slot, waiting)
    tags_copy.wait()
    for at in range(slots):
        out_copy(at).wait()


def row_constants():
    places = np.arange(SIDE) + 0.5
    rising = np.minimum(places / OVERLAP, 1.0)
    falling = np.minimum((SIDE - places) / OVERLAP, 1.0)
    columns = [rising / (SIDE * SIDE), falling]
    for order in (1, 2):
        angle = (np.arange(SIDE) * order * SHIFT_ROWS % SIDE) * (2 * math.pi / SIDE)
        columns += [np.cos(angle) / PHASES, np.sin(angle) / PHASES]
    return np.stack(columns, axis=1), np.stack([rising, falling])


def tile_results(frames, masks, phases, names, otf, apod, devices, group_count):
    slots = frames.shape[0]
    f32, bf16 = jnp.float32, jnp.bfloat16
    rows, cols = (jnp.asarray(one, f32) for one in row_constants())
    tables = [table(one) for one in (first_tables(), row_tables(), last_table())]
    places = pl.BlockSpec(memory_space=pl.ANY)

    def like(array):
        return pltpu.VMEM(array.shape, array.dtype)

    given = [frames, masks, otf, apod, rows, cols] + tables
    return pl.pallas_call(
        functools.partial(tile_kernel, devices, group_count),
        out_shape=jax.ShapeDtypeStruct((devices, TILE_GROUPS * slots + 1, GROUP, 128), bf16),
        in_specs=[pl.BlockSpec(memory_space=pltpu.SMEM)] * 2 + [places] * len(given),
        out_specs=places,
        scratch_shapes=[like(one) for one in given] + [
            pltpu.VMEM((5, SIDE, 256), f32),
            pltpu.VMEM((5 * SIDE, 256), f32),
            pltpu.VMEM((10 * SIDE, 128), f32),
            pltpu.VMEM((SIDE, 1024), f32),
            pltpu.VMEM((SIDE, 2 * SIDE), bf16),
            pltpu.VMEM((SIDE, SIDE), f32),
            pltpu.VMEM((SIDE, 256), f32),
            pltpu.VMEM((SIDE, 1920), bf16),
            pltpu.VMEM((SIDE, 1920), bf16),
            pltpu.VMEM((2 * SIDE, 1024), bf16),
            pltpu.VMEM((2 * SIDE, 256), bf16),
            pltpu.VMEM((SIDE, 256), f32),
            pltpu.VMEM((SIDE, 512), bf16),
            pltpu.VMEM((slots, devices, TILE_GROUPS, GROUP, 128), bf16),
            pltpu.VMEM((devices, 1, GROUP, 128), bf16),
            pltpu.SemaphoreType.DMA((len(given) + 2 * slots,)),
        ],
        cost_estimate=pl.CostEstimate(flops=slots * 2_000_000_000, bytes_accessed=10_000_000, transcendentals=0),
        name="tiles",
    )(names, phases, *given)


def pick_kernel(slots, devices, in_ref, out_ref, where_ref, place_ref, sem):
    me = lax.axis_index("ty")
    per_device = TILE_GROUPS * slots + 1
    line = lax.broadcasted_iota(jnp.int32, (GROUP, 128), 0)
    lane = lax.broadcasted_iota(jnp.int32, (GROUP, 128), 1).astype(jnp.float32)
    place = jnp.zeros((GROUP, 128), jnp.int32)
    for source in range(devices):
        tags = in_ref[per_device * source + per_device - 1].astype(jnp.float32)
        place += jnp.where(tags == lane, per_device * source + TILE_GROUPS * line, 0)
    where_ref[...] = jnp.sum(place, axis=0, keepdims=True)
    copy = pltpu.make_async_copy(where_ref, place_ref, sem)
    copy.start()
    copy.wait()

    for i in range(ROW_GROUPS):
        ahead = (ROW_GROUPS * me + i < OVERLAP // GROUP).astype(jnp.int32)
        for target in range(devices):
            row = target + ahead
            for col in range(GROUP_COLS):
                source = place_ref[0, GROUP_COLS * row + col] + i
                for tile in range(3):
                    value = in_ref[source + ROW_GROUPS * tile]
                    if target == devices - 1:
                        value = jnp.where(row < devices, value, jnp.zeros_like(value))
                    out_ref[TILE_GROUPS * (GROUP_COLS * target + col) + ROW_GROUPS * tile + i] = value


def picked(spread, slots):
    devices = spread.shape[0]
    chosen = pl.pallas_call(
        functools.partial(pick_kernel, slots, devices),
        out_shape=jax.ShapeDtypeStruct((devices * GROUP_COLS * TILE_GROUPS, GROUP, 128), spread.dtype),
        in_specs=[pl.BlockSpec(memory_space=pltpu.VMEM)],
        out_specs=pl.BlockSpec(memory_space=pltpu.VMEM),
        scratch_shapes=[
            pltpu.VMEM((1, 128), jnp.int32), pltpu.SMEM((1, 128), jnp.int32), pltpu.SemaphoreType.DMA,
        ],
        compiler_params=pltpu.CompilerParams(vmem_limit_bytes=SMALL_VMEM),
        name="pick",
    )(spread.reshape(-1, GROUP, 128))
    return chosen.reshape(devices, -1, GROUP, 128)


def folded(in_ref, base):
    rows = []
    for part in range(SIDE // GROUP):
        value = in_ref[part // ROW_GROUPS, base + part % ROW_GROUPS]
        rows.append(value.astype(jnp.float32))
    count = OVERLAP // GROUP
    body = rows[count:]
    for at in range(count):
        body[len(body) - count + at] = body[len(body) - count + at] + rows[at]
    return jnp.concatenate(body, axis=0)


def join_kernel(in_ref, out_ref):
    low = lax.broadcasted_iota(jnp.int32, (STRIDE, 128), 1) < OVERLAP
    left = [pltpu.roll(folded(in_ref, ROW_GROUPS * tile), OVERLAP, 1) for tile in range(3)]
    right = [folded(in_ref, TILE_GROUPS + ROW_GROUPS * tile) for tile in range(2)]
    out_ref[:, 0:128] = jnp.where(low, left[0], left[1])
    out_ref[:, 128:256] = jnp.where(low, left[1], left[2])
    out_ref[:, 256:384] = right[0] + jnp.where(low, left[2], 0.0)
    out_ref[:, 384:512] = right[1]


def join_main_kernel(in_ref, out_ref, body_ref, sem):
    join_kernel(in_ref, body_ref)
    copy = pltpu.make_async_copy(body_ref, out_ref.at[:, 0:512], sem)
    copy.start()
    copy.wait()


def edge_kernel(in_ref, strip_ref, joined_ref, out_ref, edge_ref, sem):
    low = lax.broadcasted_iota(jnp.int32, (STRIDE, 128), 1) < OVERLAP
    strip = pltpu.roll(folded(strip_ref, 0), OVERLAP, 1)
    edge_ref[...] = folded(in_ref, TILE_GROUPS + 2 * ROW_GROUPS) + jnp.where(low, 0.0, strip)
    copy = pltpu.make_async_copy(edge_ref, out_ref.at[:, 512:640], sem)
    copy.start()
    copy.wait()


def shards(frames, masks, phases, slot_tile, otf, apod):
    devices = lax.axis_size("ty")
    group_count = lax.axis_size("tx")
    slots = frames.shape[1]
    results = tile_results(
        frames[0, :, 0], masks[0][:, :, None, :], phases[:, :, 0], slot_tile, otf, apod, devices, group_count
    )
    spread = lax.all_to_all(results, "ty", 0, 0, tiled=True)
    home = lax.all_to_all(picked(spread, slots), "ty", 0, 0, tiled=True)
    strip = lax.ppermute(home[:, :ROW_GROUPS], "tx", [(g, g - 1) for g in range(1, group_count)])
    in_vmem = pl.BlockSpec(memory_space=pltpu.VMEM)
    place = jax.ShapeDtypeStruct((STRIDE, STRIDE * GROUP_COLS), jnp.float32)
    anywhere = pl.BlockSpec(memory_space=pl.ANY)
    small = pltpu.CompilerParams(vmem_limit_bytes=SMALL_VMEM)
    joined = pl.pallas_call(
        join_main_kernel, out_shape=place, in_specs=[in_vmem], out_specs=anywhere,
        scratch_shapes=[pltpu.VMEM((STRIDE, 512), jnp.float32), pltpu.SemaphoreType.DMA],
        cost_estimate=pl.CostEstimate(flops=2_000_000_000, bytes_accessed=1_400_000, transcendentals=0),
        compiler_params=small, name="join",
    )(home)
    return pl.pallas_call(
        edge_kernel, out_shape=place, in_specs=[in_vmem, in_vmem, anywhere], out_specs=anywhere,
        scratch_shapes=[pltpu.VMEM((STRIDE, 128), jnp.float32), pltpu.SemaphoreType.DMA],
        input_output_aliases={2: 0}, compiler_params=small, name="edge",
    )(home, strip, joined)


def solution(mesh):
    in_specs = (
        P("tx", "ty", None, None, None, None),
        P("tx", "ty", None, None),
        P("tx", "ty", None),
        P("tx", "ty"),
        P(),
        P(),
    )
    return jax.shard_map(
        shards, mesh=mesh, in_specs=in_specs, out_specs=P("ty", "tx"), check_vma=False
    )
```

```python
import functools
import math

import jax
import jax.numpy as jnp
import numpy as np
from jax import lax
from jax.experimental import pallas as pl
from jax.experimental.pallas import tpu as pltpu
from jax.sharding import PartitionSpec as P

SIDE = 384
STRIDE = 320
OVERLAP = SIDE - STRIDE
GROUP_COLS = 2
PHASES = 5
CELLS = 12
WIENER = 0.1
SHIFT_ROWS, SHIFT_COLS = 37, 101
CHUNK = SIDE // 16
SMALL_VMEM = 4 << 20
GROUP = 8
ROW_GROUPS = CHUNK // GROUP
TILE_GROUPS = 3 * ROW_GROUPS

NYQUIST = SIDE // 2
THIRD = SIDE // 3
HALF = SIDE // 2
BY_THREE = [np.arange(rest, HALF, 3) for rest in range(3)]


def cos_sin(rows, cols):
    angle = (np.outer(rows, cols) % SIDE) * (2.0 * math.pi / SIDE)
    return np.cos(angle), np.sin(angle)


def plus(cols):
    c, s = cos_sin(np.arange(THIRD), cols)
    return np.concatenate([c, s]), np.concatenate([-s, c])


def minus(cols):
    c, s = cos_sin(np.arange(THIRD), cols)
    return np.concatenate([c, -s]), np.concatenate([-s, -c])


def beside(blocks):
    return np.concatenate([b[0] for b in blocks] + [b[1] for b in blocks], axis=1)


def column_class(order, rest):
    return (rest - order * SHIFT_COLS) % 3


def first_tables():
    tables = []
    for order in (1, 2):
        move = order * SHIFT_COLS
        for rest in range(3):
            at = column_class(order, rest)
            if at == 0:
                blocks = [
                    plus(BY_THREE[0] + move), plus(np.array([NYQUIST + move])), minus(BY_THREE[0][1:] - move)
                ]
            elif at == 1:
                blocks = [plus(BY_THREE[1] + move), minus(BY_THREE[2] - move)]
            else:
                blocks = [minus(BY_THREE[1] - move), plus(BY_THREE[2] + move)]
            tables.append(beside(blocks))
    tables.append(beside([plus(BY_THREE[1]), minus(BY_THREE[2])]))
    blank = np.zeros((2 * THIRD, 63))
    tables.append(beside([plus(BY_THREE[0]), plus(np.array([NYQUIST])), (blank, blank)])[:THIRD])
    return np.concatenate(tables)


def row_tables():
    every = np.arange(HALF)
    tables = []
    for rows, cols in ((2 * every, every), (2 * every + 1, every)):
        c, s = cos_sin(rows, cols)
        tables.append(np.block([[c, s], [-s, c]]))
    return np.concatenate(tables)


def last_table():
    lines = np.concatenate([BY_THREE[1], BY_THREE[2], BY_THREE[0], [NYQUIST], BY_THREE[0][1:]])
    c, s = cos_sin(lines, np.arange(SIDE))
    return np.concatenate([c, s], axis=0)


def table(values):
    return jnp.asarray(values.astype(np.float32)).astype(jnp.bfloat16)


def dot(x, w):
    return jnp.dot(x, w, preferred_element_type=jnp.float32)


def halves(x):
    high = x.astype(jnp.bfloat16)
    return high, (x - high.astype(jnp.float32)).astype(jnp.bfloat16)


def negating(x_ref, flip, half_ref, back_ref):
    width = back_ref.shape[1]

    def over_rows(part):
        lanes = pl.ds(256 * part, 256)
        half_ref[:, lanes] = dot(flip, half_ref[:, lanes]).astype(jnp.bfloat16)

    def split():
        high, low = halves(x_ref[...])
        half_ref[:, 0:SIDE] = high
        half_ref[:, SIDE : 2 * SIDE] = low
        over_rows(0)

    def over_columns(low, high):
        here = flip[:, low:high]
        back_ref[:, low:high] = dot(half_ref[:, 0:SIDE], here) + dot(half_ref[:, SIDE : 2 * SIDE], here)

    steps = [split, functools.partial(over_rows, 1), functools.partial(over_rows, 2)]
    steps.append(functools.partial(over_columns, 0, 256))
    if width > 256:
        steps.append(functools.partial(over_columns, 256, width))
    return steps


def flip_matrix():
    rows = lax.broadcasted_iota(jnp.int32, (SIDE, SIDE), 0)
    cols = lax.broadcasted_iota(jnp.int32, (SIDE, SIDE), 1)
    total = rows + cols
    return ((total == 0) | (total == SIDE)).astype(jnp.float32).astype(jnp.bfloat16)


def class_matrix():
    rows = lax.broadcasted_iota(jnp.int32, (256, 256), 0)
    lane = lax.broadcasted_iota(jnp.int32, (256, 256), 1)
    wanted = jnp.where(lane < 64, 3 * lane + 1, jnp.where(lane < 128, 3 * lane - 190, 3 * lane - 384))
    wanted = jnp.where(lane == NYQUIST, NYQUIST, jnp.where(lane > NYQUIST, -1, wanted))
    return (rows == wanted).astype(jnp.float32).astype(jnp.bfloat16)


def filling(source_ref, numerator_ref, work_ref, gains_ref, first):
    def move(at):
        order = at - 2
        one = source_ref[...]
        if order:
            one = pltpu.roll(one, (-order * SHIFT_COLS) % SIDE, 1)[:, 0:256]
            one = pltpu.roll(one, (-order * SHIFT_ROWS) % SIDE, 0)
        work_ref[at] = one[:, 0:256]

    def scale(part):
        rows = pl.ds(128 * part, 128)
        power = WIENER + sum(work_ref[at, rows, :] * work_ref[at, rows, :] for at in range(5))
        weight = numerator_ref[rows, 0:256] / power
        for at in range(5):
            there = pl.ds(SIDE * at + 128 * part, 128)
            if first:
                gains_ref[there, :] = work_ref[at, rows, :] * weight
            else:
                gains_ref[there, :] += work_ref[at, rows, :] * weight

    return [functools.partial(move, at) for at in range(5)] + [functools.partial(scale, at) for at in range(3)]


def interleaved(few, many):
    done = 0
    for at, step in enumerate(few):
        step()
        until = (at + 1) * len(many) // len(few)
        for other in many[done:until]:
            other()
        done = until


def pack_gains(work_ref, gains_ref):
    lane = lax.broadcasted_iota(jnp.int32, (HALF, 128), 1)
    low = lane < 64
    nyquist = lane == 64
    for odd in range(2):
        rows = pl.ds(HALF * odd, HALF)

        def tiles(order):
            base = 2 * SIDE * (order + 2) + odd
            return tuple(work_ref[pl.ds(base + at, HALF, stride=2), :] for at in (0, SIDE))

        for order in (1, 2):
            base = 256 * (order - 1)
            up0, up1 = tiles(order)
            down0, down1 = tiles(-order)
            gains_ref[rows, base : base + 128] = jnp.where(low, up0, down0)
            gains_ref[rows, base + 128 : base + 256] = jnp.where(low, down0, up0)
            rest = jnp.where(low, up1, jnp.where(nyquist, up1, pltpu.roll(down1, 64, 1)))
            gains_ref[rows, 384 + 128 * order : 512 + 128 * order] = rest
        mid0, mid1 = tiles(0)
        gains_ref[rows, 768:896] = mid0
        edge = jnp.where(lane == 0, 0.5 * mid1, mid1)
        gains_ref[rows, 896:1024] = jnp.where(low, edge, jnp.where(nyquist, 0.5 * mid1, 0.0))


def tile_kernel(
    devices, group_count,
    names_ref, phases_ref,
    frames_hbm, masks_hbm, otf_hbm, apod_hbm, rows_hbm, cols_hbm, first_hbm, fwd_hbm, last_hbm,
    out_hbm,
    frames_ref, masks_ref, otf_ref, apod_ref, rows_ref, cols_ref, first_ref, fwd_ref, last_ref,
    work_ref, natural_ref, sorted_ref, gains_ref, half_ref, back_ref, back_apod_ref,
    left_a_ref, left_b_ref, y_ref, s_ref, t_ref, mid_ref, out_ref, tags_ref, sems,
):
    f32, bf16 = jnp.float32, jnp.bfloat16
    n1, n2 = math.sin(2 * math.pi / 5), math.sin(4 * math.pi / 5)
    slots = frames_ref.shape[0]

    fixed = [
        (otf_hbm, otf_ref), (apod_hbm, apod_ref), (masks_hbm, masks_ref), (rows_hbm, rows_ref),
        (cols_hbm, cols_ref), (first_hbm, first_ref), (fwd_hbm, fwd_ref), (last_hbm, last_ref),
    ]
    early = 5
    left_refs = (left_a_ref, left_b_ref)

    def fixed_copy(at):
        return pltpu.make_async_copy(fixed[at][0], fixed[at][1], sems.at[at])

    def frame_copy(at):
        return pltpu.make_async_copy(frames_hbm.at[at], frames_ref.at[at], sems.at[len(fixed) + at])

    def out_copy(at):
        there = out_hbm.at[:, pl.ds(TILE_GROUPS * at, TILE_GROUPS)]
        return pltpu.make_async_copy(out_ref.at[at], there, sems.at[len(fixed) + slots + at])

    tags_copy = pltpu.make_async_copy(
        tags_ref, out_hbm.at[:, pl.ds(TILE_GROUPS * slots, 1)], sems.at[len(fixed) + 2 * slots]
    )

    def mixing(now):
        phase = jnp.full((GROUP, 128), phases_ref[0, now], f32)
        turns = [[fn(order * phase)[0:1, 0:1] for fn in (jnp.cos, jnp.sin)] for order in (1.0, 2.0)]
        cell_row = lax.broadcasted_iota(jnp.int32, (CELLS, SIDE), 0)
        cell_col = lax.broadcasted_iota(jnp.int32, (CELLS, SIDE), 1) // (SIDE // CELLS)
        spread = (cell_row == cell_col).astype(f32).astype(bf16)
        held = jnp.concatenate([masks_ref[now, row] for row in range(CELLS)], axis=0)
        flags = dot(held.astype(f32).astype(bf16), spread)

        def thirds(x):
            a, b, c = x[:, 0:128], x[:, 128:256], x[:, 256:384]
            both = b + c
            return a + both, a - 0.5 * both, (0.5 * math.sqrt(3.0)) * (b - c)

        def step(part):
            rows = pl.ds(64 * part, 64)
            flag = jnp.concatenate([jnp.broadcast_to(flags[2 * part + at : 2 * part + at + 1, :], (32, SIDE)) for at in range(2)], axis=0).astype(bf16)
            f = [(frames_ref[now, p, rows, :] * flag).astype(f32) for p in range(PHASES)]
            a1, d1, a2, d2 = f[1] + f[4], f[1] - f[4], f[2] + f[3], f[2] - f[3]

            def put(at, value):
                left_refs[now % 2][rows, 128 * at : 128 * at + 128] = value.astype(bf16)

            both = a1 + a2
            total, even, odd = thirds((f[0] + both) * (1.0 / PHASES))
            base, apart = f[0] - 0.25 * both, (0.25 * math.sqrt(5.0)) * (a1 - a2)
            put(12, even)
            put(13, -odd)
            put(14, total)
            for at, (a, b) in enumerate((
                (base + apart, n1 * d1 + n2 * d2),
                (base - apart, n2 * d1 - n1 * d2),
            )):
                turn_c, turn_s = turns[at]
                row_c, row_s = rows_ref[rows, 2 + 2 * at : 3 + 2 * at], rows_ref[rows, 3 + 2 * at : 4 + 2 * at]
                c = turn_c * row_c - turn_s * row_s
                s = turn_s * row_c + turn_c * row_s
                total_r, even_r, odd_r = thirds(c * a - s * b)
                total_i, even_i, odd_i = thirds(-c * b - s * a)
                put(6 * at, total_r)
                put(6 * at + 1, total_i)
                put(6 * at + 2, even_r + odd_i)
                put(6 * at + 3, even_i - odd_r)
                put(6 * at + 4, even_r - odd_i)
                put(6 * at + 5, even_i + odd_r)

        return [functools.partial(step, part) for part in range(CELLS // 2)]

    def transform(slot, waiting):
        def mix_some(count):
            for step in waiting[:count]:
                step()
            del waiting[:count]

        def put_rows(r, col):
            for half in range(2):
                top = r[0:HALF, 128 * half : 128 * half + 128]
                bottom = r[HALF:SIDE, 128 * half : 128 * half + 128]
                base = HALF * half
                y_ref[base : base + HALF, col : col + 128] = (top + bottom).astype(bf16)
                y_ref[SIDE + base : SIDE + base + HALF, col : col + 128] = (top - bottom).astype(bf16)

        for at in range(2):
            columns = (512 + 128 * at, 256 * at, 256 * at + 128)
            for rest in range(3):
                k = 768 * at + 256 * rest
                r = dot(left_refs[slot % 2][:, k : k + 256], first_ref[k : k + 256, :])
                put_rows(r, columns[column_class(at + 1, rest)])
                mix_some(1)
        put_rows(dot(left_refs[slot % 2][:, 1536:1792], first_ref[1536:1792, :]), 768)
        mix_some(1)
        put_rows(dot(left_refs[slot % 2][:, 1792:1920], first_ref[1792:1920, :]), 896)
        mix_some(1)

        for odd in range(2):
            rows = pl.ds(SIDE * odd, SIDE)
            gain_rows = pl.ds(HALF * odd, HALF)
            for n in range(4):
                lanes = pl.ds(256 * n, 256)
                product = dot(fwd_ref[rows, :], y_ref[rows, lanes])
                g = gains_ref[gain_rows, lanes]
                for half in range(2):
                    d = product[HALF * half : HALF * half + HALF] * g
                    here = pl.ds(HALF * half, HALF)
                    if n == 0:
                        t_ref[here, 0:128] = d[:, 0:128] + d[:, 128:256]
                    elif n == 1:
                        t_ref[here, 0:128] += d[:, 0:128] + d[:, 128:256]
                    elif n == 2:
                        t_ref[here, 128:256] = d[:, 0:128] + d[:, 128:256]
                    else:
                        total = t_ref[here, :] + d
                        total = -total if half > odd else total
                        base = SIDE * odd + HALF * half
                        s_ref[base : base + HALF, :] = total.astype(bf16)
                mix_some(1 if n % 2 else 0)

        even_part = dot(fwd_ref[0:SIDE, :], s_ref[0:SIDE, :])
        odd_part = lax.dot_general(
            fwd_ref[SIDE : 2 * SIDE, :], s_ref[SIDE : 2 * SIDE, :], (((0,), (0,)), ((), ())),
            preferred_element_type=f32,
        )
        mix_some(len(waiting))
        for half in range(2):
            e, o = even_part[HALF * half : HALF * half + HALF], odd_part[HALF * half : HALF * half + HALF]
            o = -o if half else o
            lanes = pl.ds(256 * half, 256)
            mid_ref[0:HALF, lanes] = (e + o).astype(bf16)
            mid_ref[HALF:SIDE, lanes] = (e - o).astype(bf16)
        picture = dot(mid_ref[...], last_ref[...])
        name = names_ref[0, slot]
        row_last = name >= GROUP_COLS * (devices - 1)
        col_last = (lax.axis_index("tx") == group_count - 1) & (lax.rem(name, GROUP_COLS) == GROUP_COLS - 1)
        row_ramp = rows_ref[:, 0:1] * jnp.where(row_last, 1.0, rows_ref[:, 1:2])
        col_ramp = cols_ref[0:1, :] * jnp.where(col_last, 1.0, cols_ref[1:2, :])
        weighted = picture * row_ramp * col_ramp
        for part in range(SIDE // GROUP):
            chunk, i = part // ROW_GROUPS, part % ROW_GROUPS
            for tile in range(3):
                piece = weighted[GROUP * part : GROUP * part + GROUP, 128 * tile : 128 * tile + 128]
                out_ref[slot, chunk, ROW_GROUPS * tile + i] = piece.astype(bf16)
        out_copy(slot).start()

    for at in range(early):
        fixed_copy(at).start()
    frame_copy(0).start()
    line = lax.broadcasted_iota(jnp.int32, (GROUP, 128), 0)
    tags = jnp.full((GROUP, 128), -1.0, f32)
    for at in range(slots):
        tags = jnp.where(line == at, names_ref[0, at].astype(f32), tags)
    for chunk in range(devices):
        tags_ref[chunk, 0] = tags.astype(bf16)
    tags_copy.start()
    flip = flip_matrix()
    for at in range(early):
        fixed_copy(at).wait()
    for at in range(early, len(fixed)):
        fixed_copy(at).start()
    turning = negating(otf_ref, flip, half_ref, back_ref)
    interleaved(turning, filling(otf_ref, apod_ref, work_ref, natural_ref, True))
    frame_copy(0).wait()
    for at in range(1, slots):
        frame_copy(at).start()
    interleaved(negating(apod_ref, flip, half_ref, back_apod_ref), mixing(0))
    for step in filling(back_ref, back_apod_ref, work_ref, natural_ref, False):
        step()
    classes = class_matrix()
    for at in range(5):
        rows = pl.ds(SIDE * at, SIDE)
        high, low = halves(natural_ref[rows, :])
        sorted_gains = dot(high, classes) + dot(low, classes)
        for half in range(2):
            there = pl.ds(SIDE * (2 * at + half), SIDE)
            sorted_ref[there, :] = sorted_gains[:, 128 * half : 128 * half + 128]
    pack_gains(sorted_ref, gains_ref)
    for at in range(early, len(fixed)):
        fixed_copy(at).wait()

    for slot in range(slots):
        waiting = []
        if slot + 1 < slots:
            frame_copy(slot + 1).wait()
            waiting = mixing(slot + 1)
        transform(slot, waiting)
    tags_copy.wait()
    for at in range(slots):
        out_copy(at).wait()


def row_constants():
    places = np.arange(SIDE) + 0.5
    rising = np.minimum(places / OVERLAP, 1.0)
    falling = np.minimum((SIDE - places) / OVERLAP, 1.0)
    columns = [rising / (SIDE * SIDE), falling]
    for order in (1, 2):
        angle = (np.arange(SIDE) * order * SHIFT_ROWS % SIDE) * (2 * math.pi / SIDE)
        columns += [np.cos(angle) / PHASES, np.sin(angle) / PHASES]
    return np.stack(columns, axis=1), np.stack([rising, falling])


def tile_results(frames, masks, phases, names, otf, apod, devices, group_count):
    slots = frames.shape[0]
    f32, bf16 = jnp.float32, jnp.bfloat16
    rows, cols = (jnp.asarray(one, f32) for one in row_constants())
    tables = [table(one) for one in (first_tables(), row_tables(), last_table())]
    places = pl.BlockSpec(memory_space=pl.ANY)

    def like(array):
        return pltpu.VMEM(array.shape, array.dtype)

    given = [frames, masks, otf, apod, rows, cols] + tables
    return pl.pallas_call(
        functools.partial(tile_kernel, devices, group_count),
        out_shape=jax.ShapeDtypeStruct((devices, TILE_GROUPS * slots + 1, GROUP, 128), bf16),
        in_specs=[pl.BlockSpec(memory_space=pltpu.SMEM)] * 2 + [places] * len(given),
        out_specs=places,
        scratch_shapes=[like(one) for one in given] + [
            pltpu.VMEM((5, SIDE, 256), f32),
            pltpu.VMEM((5 * SIDE, 256), f32),
            pltpu.VMEM((10 * SIDE, 128), f32),
            pltpu.VMEM((SIDE, 1024), f32),
            pltpu.VMEM((SIDE, 2 * SIDE), bf16),
            pltpu.VMEM((SIDE, SIDE), f32),
            pltpu.VMEM((SIDE, 256), f32),
            pltpu.VMEM((SIDE, 1920), bf16),
            pltpu.VMEM((SIDE, 1920), bf16),
            pltpu.VMEM((2 * SIDE, 1024), bf16),
            pltpu.VMEM((2 * SIDE, 256), bf16),
            pltpu.VMEM((SIDE, 256), f32),
            pltpu.VMEM((SIDE, 512), bf16),
            pltpu.VMEM((slots, devices, TILE_GROUPS, GROUP, 128), bf16),
            pltpu.VMEM((devices, 1, GROUP, 128), bf16),
            pltpu.SemaphoreType.DMA((len(given) + 2 * slots,)),
        ],
        cost_estimate=pl.CostEstimate(flops=slots * 2_000_000_000, bytes_accessed=10_000_000, transcendentals=0),
        name="tiles",
    )(names, phases, *given)


def pick_kernel(slots, devices, in_ref, out_ref, where_ref, place_ref, sem):
    me = lax.axis_index("ty")
    per_device = TILE_GROUPS * slots + 1
    line = lax.broadcasted_iota(jnp.int32, (GROUP, 128), 0)
    lane = lax.broadcasted_iota(jnp.int32, (GROUP, 128), 1).astype(jnp.float32)
    place = jnp.zeros((GROUP, 128), jnp.int32)
    for source in range(devices):
        tags = in_ref[per_device * source + per_device - 1].astype(jnp.float32)
        place += jnp.where(tags == lane, per_device * source + TILE_GROUPS * line, 0)
    where_ref[...] = jnp.sum(place, axis=0, keepdims=True)
    copy = pltpu.make_async_copy(where_ref, place_ref, sem)
    copy.start()
    copy.wait()

    for i in range(ROW_GROUPS):
        ahead = (ROW_GROUPS * me + i < OVERLAP // GROUP).astype(jnp.int32)
        for target in range(devices):
            row = target + ahead
            for col in range(GROUP_COLS):
                source = place_ref[0, GROUP_COLS * row + col] + i
                for tile in range(3):
                    value = in_ref[source + ROW_GROUPS * tile]
                    if target == devices - 1:
                        value = jnp.where(row < devices, value, jnp.zeros_like(value))
                    out_ref[TILE_GROUPS * (GROUP_COLS * target + col) + ROW_GROUPS * tile + i] = value


def picked(spread, slots):
    devices = spread.shape[0]
    chosen = pl.pallas_call(
        functools.partial(pick_kernel, slots, devices),
        out_shape=jax.ShapeDtypeStruct((devices * GROUP_COLS * TILE_GROUPS, GROUP, 128), spread.dtype),
        in_specs=[pl.BlockSpec(memory_space=pltpu.VMEM)],
        out_specs=pl.BlockSpec(memory_space=pltpu.VMEM),
        scratch_shapes=[
            pltpu.VMEM((1, 128), jnp.int32), pltpu.SMEM((1, 128), jnp.int32), pltpu.SemaphoreType.DMA,
        ],
        compiler_params=pltpu.CompilerParams(vmem_limit_bytes=SMALL_VMEM),
        name="pick",
    )(spread.reshape(-1, GROUP, 128))
    return chosen.reshape(devices, -1, GROUP, 128)


def folded(in_ref, base):
    rows = []
    for part in range(SIDE // GROUP):
        value = in_ref[part // ROW_GROUPS, base + part % ROW_GROUPS]
        rows.append(value.astype(jnp.float32))
    count = OVERLAP // GROUP
    body = rows[count:]
    for at in range(count):
        body[len(body) - count + at] = body[len(body) - count + at] + rows[at]
    return jnp.concatenate(body, axis=0)


def join_kernel(in_ref, out_ref):
    low = lax.broadcasted_iota(jnp.int32, (STRIDE, 128), 1) < OVERLAP
    left = [pltpu.roll(folded(in_ref, ROW_GROUPS * tile), OVERLAP, 1) for tile in range(3)]
    right = [folded(in_ref, TILE_GROUPS + ROW_GROUPS * tile) for tile in range(2)]
    out_ref[:, 0:128] = jnp.where(low, left[0], left[1])
    out_ref[:, 128:256] = jnp.where(low, left[1], left[2])
    out_ref[:, 256:384] = right[0] + jnp.where(low, left[2], 0.0)
    out_ref[:, 384:512] = right[1]


def join_main_kernel(in_ref, out_ref, body_ref, sem):
    join_kernel(in_ref, body_ref)
    copy = pltpu.make_async_copy(body_ref, out_ref.at[:, 0:512], sem)
    copy.start()
    copy.wait()


def edge_kernel(in_ref, strip_ref, joined_ref, out_ref, edge_ref, sem):
    low = lax.broadcasted_iota(jnp.int32, (STRIDE, 128), 1) < OVERLAP
    strip = pltpu.roll(folded(strip_ref, 0), OVERLAP, 1)
    edge_ref[...] = folded(in_ref, TILE_GROUPS + 2 * ROW_GROUPS) + jnp.where(low, 0.0, strip)
    copy = pltpu.make_async_copy(edge_ref, out_ref.at[:, 512:640], sem)
    copy.start()
    copy.wait()


def shards(frames, masks, phases, slot_tile, otf, apod):
    devices = lax.axis_size("ty")
    group_count = lax.axis_size("tx")
    slots = frames.shape[1]
    results = tile_results(
        frames[0, :, 0], masks[0][:, :, None, :], phases[:, :, 0], slot_tile, otf, apod, devices, group_count
    )
    spread = lax.all_to_all(results, "ty", 0, 0, tiled=True)
    home = lax.all_to_all(picked(spread, slots), "ty", 0, 0, tiled=True)
    strip = lax.ppermute(home[:, :ROW_GROUPS], "tx", [(g, g - 1) for g in range(1, group_count)])
    in_vmem = pl.BlockSpec(memory_space=pltpu.VMEM)
    place = jax.ShapeDtypeStruct((STRIDE, STRIDE * GROUP_COLS), jnp.float32)
    anywhere = pl.BlockSpec(memory_space=pl.ANY)
    small = pltpu.CompilerParams(vmem_limit_bytes=SMALL_VMEM)
    joined = pl.pallas_call(
        join_main_kernel, out_shape=place, in_specs=[in_vmem], out_specs=anywhere,
        scratch_shapes=[pltpu.VMEM((STRIDE, 512), jnp.float32), pltpu.SemaphoreType.DMA],
        cost_estimate=pl.CostEstimate(flops=2_000_000_000, bytes_accessed=1_400_000, transcendentals=0),
        compiler_params=small, name="join",
    )(home)
    return pl.pallas_call(
        edge_kernel, out_shape=place, in_specs=[in_vmem, in_vmem, anywhere], out_specs=anywhere,
        scratch_shapes=[pltpu.VMEM((STRIDE, 128), jnp.float32), pltpu.SemaphoreType.DMA],
        input_output_aliases={2: 0}, compiler_params=small, name="edge",
    )(home, strip, joined)


def solution(mesh):
    in_specs = (
        P("tx", "ty", None, None, None, None),
        P("tx", "ty", None, None),
        P("tx", "ty", None),
        P("tx", "ty"),
        P(),
        P(),
    )
    return jax.shard_map(
        shards, mesh=mesh, in_specs=in_specs, out_specs=P("ty", "tx"), check_vma=False
    )
```
